128 devices in a mesh: tp: 2 (over core), dp: 64 (over z, y, x).
Axes of the slice: x: 4, y: 4, z: 4, core: 2. Of those that a mesh axis runs over, the one named last changes fastest.
Arguments:
- hidden: bfloat16 [64, 512, 6144], P('dp')
- gain_in: float32 [6144], replicated
- gain_q: float32 [1536], replicated
- gain_kv: float32 [512], replicated
- w_qa: bfloat16 [6144, 1536], replicated
- w_kva: bfloat16 [6144, 576], replicated
- w_qb: bfloat16 [1536, 12288], P(None, 'tp')
- w_kvb: bfloat16 [512, 16384], P(None, 'tp')
- w_out: bfloat16 [8192, 6144], P('tp')
Outputs:
- output 1: bfloat16 [64, 512, 6144], P('dp')
- output 2: float32 [64], replicated
- output 3: bfloat16 [1536, 12288], P(None, 'tp')
- output 4: bfloat16 [512, 16384], P(None, 'tp')
All inputs are finite; a program needn't handle non-finite values.
Results may differ from the reference program's by a relative error of at most 0.00727773.
Values sent between devices are 32-bit elements.
A program may use at most 1 GiB of HBM per device.

```python
import math
import jax
import jax.numpy as jnp
from jax import lax

B_ALL = 64
SEQ_LEN = 512
D = 6144
HEADS = 64
Q_LORA = 1536
KV_LORA = 512
NOPE_DIM = 128
ROPE_DIM = 64
V_DIM = 128
CLIP_TAU = 100

QK_DIM = NOPE_DIM + ROPE_DIM
NORM_EPS = 1e-6
ROPE_BASE = 50000.0
MSCALE_SQ = (0.1 * math.log(32.0) + 1.0) ** 2
LOGIT_SCALE = QK_DIM ** -0.5 * MSCALE_SQ


def rms_norm(tensor, gain_vec):
    return tensor * lax.rsqrt(jnp.mean(tensor * tensor, axis=-1, keepdims=True) + NORM_EPS) * gain_vec


def rotate(tensor, cos_table, sin_table):
    half_dim = ROPE_DIM // 2
    first_half = tensor[..., :half_dim]
    second_half = tensor[..., half_dim:]
    return jnp.concatenate([first_half * cos_table - second_half * sin_table, first_half * sin_table + second_half * cos_table], axis=-1)


def column_gains(first_gain, first_dim, second_gain, second_dim):
    return jnp.concatenate([jnp.broadcast_to(first_gain[:, None], (HEADS, first_dim)), jnp.broadcast_to(second_gain[:, None], (HEADS, second_dim))], axis=1).reshape(-1)


def setup_inputs(seed: int = 0) -> dict:
    key_list = jax.random.split(jax.random.key(seed), 14)
    common = jax.random.normal(key_list[0], (B_ALL, 1, D), jnp.float32)
    noise_part = jax.random.normal(key_list[1], (B_ALL, SEQ_LEN, D), jnp.float32)
    free_draw = jax.random.randint(key_list[2], (B_ALL,), 0, 64)
    free_pick = jax.random.randint(key_list[3], (), 0, B_ALL)
    independent = (free_draw == 0) | (jnp.arange(B_ALL) == free_pick)
    share_w = jnp.where(independent, 0.0, 0.9)[:, None, None]
    hidden = (share_w * common + jnp.sqrt(1.0 - share_w * share_w) * noise_part).astype(jnp.bfloat16)
    gain_in = 1.0 + 0.2 * jax.random.normal(key_list[4], (D,), jnp.float32)
    gain_q = 1.0 + 0.2 * jax.random.normal(key_list[5], (Q_LORA,), jnp.float32)
    gain_kv = 1.0 + 0.2 * jax.random.normal(key_list[6], (KV_LORA,), jnp.float32)
    w_qa = (jax.random.normal(key_list[7], (D, Q_LORA), jnp.float32) * D ** -0.5).astype(jnp.bfloat16)
    w_kva = (jax.random.normal(key_list[8], (D, KV_LORA + ROPE_DIM), jnp.float32) * D ** -0.5).astype(jnp.bfloat16)
    target = CLIP_TAU / (MSCALE_SQ * math.sqrt(2.0 * math.log(0.5 * SEQ_LEN * SEQ_LEN)))
    head_scale = jnp.exp(jax.random.uniform(key_list[9], (HEADS,), jnp.float32, math.log(0.5), math.log(2.5))) * target
    w_qb = (jax.random.normal(key_list[10], (Q_LORA, HEADS, QK_DIM), jnp.float32) * head_scale[None, :, None] * Q_LORA ** -0.5).reshape(Q_LORA, HEADS * QK_DIM).astype(jnp.bfloat16)
    w_kvb = (jax.random.normal(key_list[11], (KV_LORA, HEADS * (NOPE_DIM + V_DIM)), jnp.float32) * KV_LORA ** -0.5).astype(jnp.bfloat16)
    w_out = (jax.random.normal(key_list[12], (HEADS * V_DIM, D), jnp.float32) * (HEADS * V_DIM) ** -0.5).astype(jnp.bfloat16)
    return {'hidden': hidden, 'gain_in': gain_in, 'gain_q': gain_q, 'gain_kv': gain_kv, 'w_qa': w_qa, 'w_kva': w_kva, 'w_qb': w_qb, 'w_kvb': w_kvb, 'w_out': w_out}


def reference(hidden, gain_in, gain_q, gain_kv, w_qa, w_kva, w_qb, w_kvb, w_out):
    positions = jnp.arange(SEQ_LEN, dtype=jnp.float32)
    inv_freq = ROPE_BASE ** (-2.0 * jnp.arange(ROPE_DIM // 2, dtype=jnp.float32) / ROPE_DIM)
    angles = positions[:, None] * inv_freq[None, :]
    cos_table = jnp.cos(angles)
    sin_table = jnp.sin(angles)
    causal = jnp.arange(SEQ_LEN)[:, None] >= jnp.arange(SEQ_LEN)[None, :]

    def per_sequence(tokens):
        normed = rms_norm(tokens.astype(jnp.float32), gain_in).astype(jnp.bfloat16)
        q_lat = rms_norm(jnp.dot(normed, w_qa, preferred_element_type=jnp.float32), gain_q).astype(jnp.bfloat16)
        kv_lat = jnp.dot(normed, w_kva, preferred_element_type=jnp.float32)
        latent = rms_norm(kv_lat[:, :KV_LORA], gain_kv).astype(jnp.bfloat16)
        k_rot = rotate(kv_lat[:, KV_LORA:], cos_table, sin_table).astype(jnp.bfloat16)
        q_full = jnp.dot(q_lat, w_qb, preferred_element_type=jnp.float32).reshape(SEQ_LEN, HEADS, QK_DIM)
        q_nope = q_full[..., :NOPE_DIM].astype(jnp.bfloat16)
        q_rot = rotate(q_full[..., NOPE_DIM:], cos_table[:, None, :], sin_table[:, None, :]).astype(jnp.bfloat16)
        kv_full = jnp.dot(latent, w_kvb, preferred_element_type=jnp.float32).astype(jnp.bfloat16).reshape(SEQ_LEN, HEADS, NOPE_DIM + V_DIM)
        k_nope = kv_full[..., :NOPE_DIM].astype(jnp.float32)
        values = kv_full[..., NOPE_DIM:].astype(jnp.float32)
        logits = jnp.einsum('qhd,khd->hqk', q_nope.astype(jnp.float32), k_nope) + jnp.einsum('qhd,kd->hqk', q_rot.astype(jnp.float32), k_rot.astype(jnp.float32))
        logits = jnp.where(causal[None], logits * LOGIT_SCALE, -jnp.inf)
        attn_prob = jax.nn.softmax(logits, axis=-1).astype(jnp.bfloat16)
        attn_out = jnp.einsum('hqk,khd->qhd', attn_prob.astype(jnp.float32), values).astype(jnp.bfloat16).reshape(SEQ_LEN, HEADS * V_DIM)
        update = jnp.dot(attn_out, w_out, preferred_element_type=jnp.float32)
        return (tokens.astype(jnp.float32) + update).astype(jnp.bfloat16), jnp.max(logits, axis=(1, 2))

    out_hidden, seq_max = lax.map(per_sequence, hidden)
    logit_max = jnp.max(seq_max, axis=0)
    clip_gain = CLIP_TAU / jnp.maximum(CLIP_TAU, logit_max)
    root_gain = jnp.sqrt(clip_gain)
    new_qb = (w_qb.astype(jnp.float32) * column_gains(root_gain, NOPE_DIM, clip_gain, ROPE_DIM)[None, :]).astype(jnp.bfloat16)
    new_kvb = (w_kvb.astype(jnp.float32) * column_gains(root_gain, NOPE_DIM, jnp.ones_like(clip_gain), V_DIM)[None, :]).astype(jnp.bfloat16)
    return out_hidden, logit_max, new_qb, new_kvb
```

```python
import math
import jax
import jax.numpy as jnp
from jax import lax
from jax.experimental import pallas as pl
from jax.experimental.pallas import tpu as pltpu
from jax.sharding import PartitionSpec as P

NORM_EPS = 1e-6
ROPE_BASE = 50000.0
MSCALE_SQ = (0.1 * math.log(32.0) + 1.0) ** 2
CLIP_TAU = 100.0
NOPE, ROPE, VDIM = 128, 64, 128
QK = NOPE + ROPE
LOGIT_SCALE = QK ** -0.5 * MSCALE_SQ
EXP2_SCALE = LOGIT_SCALE * math.log2(math.e)
GROUP = 4
NEG = -jnp.inf
MESH = pl.DeviceIdType.MESH
VMEM_MAX = 63 * 1024 * 1024
f32, bf16 = jnp.float32, jnp.bfloat16


def rope_tables(seq_len):
    inv_freq = ROPE_BASE ** (-2.0 * jnp.arange(ROPE // 2, dtype=f32) / ROPE)
    angles = jnp.arange(seq_len).astype(f32)[:, None] * inv_freq[None, :]
    cos, sin = jnp.cos(angles), jnp.sin(angles)
    one, zero = jnp.ones((seq_len, ROPE), f32), jnp.zeros((seq_len, ROPE), f32)
    half = jnp.zeros_like(sin)
    keep, low, high = (cos, cos), (-sin, half), (half, sin)
    first = [jnp.concatenate([*t, pad], axis=1) for t, pad in ((keep, one), (low, zero), (high, zero))]
    second = [jnp.concatenate([pad, *t], axis=1) for t, pad in ((keep, one), (low, zero), (high, zero))]
    return jnp.stack(first + second)


def turn(tensor, tables, start):
    return tensor * tables[start] + pltpu.roll(tensor, 96, 1) * tables[start + 1] + pltpu.roll(tensor, 32, 1) * tables[start + 2]


def latent_kernel(x_ref, gin_ref, gq_ref, gkv_ref, wqa_ref, wkva_ref, tab_ref, qlat_ref, lat_ref, kr_ref, scale_ref, accq_ref, acckv_ref):
    step, steps = pl.program_id(0), pl.num_programs(0)
    depth = wqa_ref.shape[0]
    rows, dim = x_ref.shape

    @pl.when(step == 0)
    def _():
        for r in range(0, rows, 64):
            total = jnp.zeros((64, 128), f32)
            for c in range(0, dim, 128):
                v = x_ref[r:r + 64, c:c + 128].astype(f32)
                total = total + v * v
            mean = jnp.sum(total, axis=1, keepdims=True) * (1.0 / dim)
            scale_ref[r:r + 64, :] = jnp.broadcast_to(lax.rsqrt(mean + NORM_EPS), (64, 128))

    start = pl.multiple_of(step * depth, depth)
    n = (x_ref[:, pl.ds(start, depth)].astype(f32) * scale_ref[:, 0:1] * gin_ref[:, pl.ds(start, depth)]).astype(bf16)
    pq = jnp.dot(n, wqa_ref[...], preferred_element_type=f32)
    pkv = jnp.dot(n, wkva_ref[...], preferred_element_type=f32)

    @pl.when(step == 0)
    def _():
        accq_ref[...] = pq
        acckv_ref[...] = pkv

    @pl.when(step > 0)
    def _():
        accq_ref[...] += pq
        acckv_ref[...] += pkv

    @pl.when(step == steps - 1)
    def _():
        q = accq_ref[...]
        qlat_ref[...] = (q * lax.rsqrt(jnp.mean(q * q, axis=1, keepdims=True) + NORM_EPS) * gq_ref[...]).astype(bf16)
        rank = lat_ref.shape[1]
        a = acckv_ref[:, :rank]
        lat_ref[...] = (a * lax.rsqrt(jnp.mean(a * a, axis=1, keepdims=True) + NORM_EPS) * gkv_ref[...]).astype(bf16)
        key = jnp.concatenate([acckv_ref[:, rank:rank + ROPE], jnp.zeros((rows, ROPE), f32)], axis=1)
        key = turn(key, tab_ref, 0)
        kr_ref[0] = key.astype(bf16)
        kr_ref[1] = pltpu.roll(key, 64, 1).astype(bf16)


def latents(x, gin, gq, gkv, wqa, wkva, tables):
    rows, dim = x.shape
    q_rank, kva, rank = wqa.shape[1], wkva.shape[1], gkv.shape[1]
    depth = 768
    whole = lambda shape: pl.BlockSpec(shape, lambda k: (0,) * len(shape), pipeline_mode=pl.Buffered(1))
    return pl.pallas_call(
        latent_kernel,
        grid=(dim // depth,),
        in_specs=[whole(x.shape), whole(gin.shape), whole(gq.shape), whole(gkv.shape), pl.BlockSpec((depth, q_rank), lambda k: (k, 0)), pl.BlockSpec((depth, kva), lambda k: (k, 0)), whole(tables.shape)],
        out_specs=[whole((rows, q_rank)), whole((rows, rank)), whole((2, rows, 128))],
        out_shape=[jax.ShapeDtypeStruct((rows, q_rank), bf16), jax.ShapeDtypeStruct((rows, rank), bf16), jax.ShapeDtypeStruct((2, rows, 128), bf16)],
        scratch_shapes=[pltpu.VMEM((rows, 128), f32), pltpu.VMEM((rows, q_rank), f32), pltpu.VMEM((rows, kva), f32)],
        compiler_params=pltpu.CompilerParams(vmem_limit_bytes=VMEM_MAX),
        name="latents",
    )(x, gin, gq, gkv, wqa, wkva, tables)


def attend(q, key, value, out_ref, column):
    rows = q.shape[0]
    block = 256
    best = None
    for b in range(rows // block):
        lo, hi = b * block, (b + 1) * block
        raw = lax.dot_general(q[lo:hi], key[:hi], (((1,), (1,)), ((), ())), preferred_element_type=f32)
        keep = lax.broadcasted_iota(jnp.int32, (block, block), 0) >= lax.broadcasted_iota(jnp.int32, (block, block), 1)
        last = jnp.where(keep, raw[:, lo:hi], NEG)
        raw = last if b == 0 else jnp.concatenate([raw[:, :lo], last], axis=1)
        top = jnp.max(raw, axis=1, keepdims=True)
        e = jnp.exp2(raw * EXP2_SCALE - top * EXP2_SCALE)
        p = (e * (1.0 / jnp.sum(e, axis=1, keepdims=True))).astype(bf16)
        out_ref[lo:hi, column:column + VDIM] = jnp.dot(p, value[:hi], preferred_element_type=f32).astype(bf16)
        peak = jnp.max(top, axis=0, keepdims=True)
        best = peak if best is None else jnp.maximum(best, peak)
    return best


def attention_kernel(qlat_ref, lat_ref, kr_ref, tab_ref, wqb_ref, wkvb_ref, o_ref, max_ref):
    group = pl.program_id(0)
    heads = pl.num_programs(0) * GROUP
    first = lax.axis_index("tp") * heads + group * GROUP
    q_all = jnp.dot(qlat_ref[...], wqb_ref[...], preferred_element_type=f32)
    kv_all = jnp.dot(lat_ref[...], wkvb_ref[...], preferred_element_type=f32)
    rows = q_all.shape[0]
    lane = lax.broadcasted_iota(jnp.int32, (rows, 128), 1)
    slot = lax.broadcasted_iota(jnp.int32, (8, 128), 1)

    @pl.when(group == 0)
    def _():
        max_ref[...] = jnp.full((8, 128), NEG, f32)

    found = max_ref[...]
    for pair in range(GROUP // 2):
        qc, kc = pair * 2 * QK, pair * 2 * (NOPE + VDIM)
        part_a = q_all[:, qc:qc + 128].astype(bf16)
        part_b = turn(q_all[:, qc + 128:qc + 256], tab_ref, 0).astype(bf16)
        part_c = turn(q_all[:, qc + 256:qc + 384], tab_ref, 3).astype(bf16)
        for odd in range(2):
            kcol = kc + odd * (NOPE + VDIM)
            nope = kv_all[:, kcol:kcol + NOPE]
            value = kv_all[:, kcol + NOPE:kcol + NOPE + VDIM].astype(bf16)
            if odd:
                moved = pltpu.roll(nope, 64, 1)
                q = jnp.concatenate([part_b, part_c], axis=1)
                key = jnp.concatenate([jnp.where(lane >= 64, moved, 0.0).astype(bf16), jnp.where(lane < 64, moved.astype(bf16), kr_ref[1])], axis=1)
            else:
                q = jnp.concatenate([part_a, part_b], axis=1)
                key = jnp.concatenate([nope.astype(bf16), kr_ref[0]], axis=1)
            best = attend(q, key, value, o_ref, (pair * 2 + odd) * VDIM)
            found = jnp.where(slot == first + pair * 2 + odd, best * LOGIT_SCALE, found)
    max_ref[...] = found


def attention(qlat, lat, kr, tables, wqb, wkvb):
    rows = qlat.shape[0]
    heads = wqb.shape[1] // QK
    whole = lambda shape: pl.BlockSpec(shape, lambda g: (0,) * len(shape), pipeline_mode=pl.Buffered(1))
    return pl.pallas_call(
        attention_kernel,
        grid=(heads // GROUP,),
        in_specs=[whole(qlat.shape), whole(lat.shape), whole(kr.shape), whole(tables.shape), pl.BlockSpec((wqb.shape[0], GROUP * QK), lambda g: (0, g)), pl.BlockSpec((wkvb.shape[0], GROUP * (NOPE + VDIM)), lambda g: (0, g))],
        out_specs=[pl.BlockSpec((rows, GROUP * VDIM), lambda g: (0, g)), pl.BlockSpec((8, 128), lambda g: (0, 0))],
        out_shape=[jax.ShapeDtypeStruct((rows, heads * VDIM), bf16), jax.ShapeDtypeStruct((8, 128), f32)],
        compiler_params=pltpu.CompilerParams(vmem_limit_bytes=VMEM_MAX),
        name="attention",
    )(qlat, lat, kr, tables, wqb, wkvb)


def axis_peers(axis):
    dp = lax.axis_index("dp")
    stride = 4 ** axis
    here = lax.rem(dp // stride, 4)
    return [dp + (lax.rem(here + d, 4) - here) * stride for d in (1, 2, 3)]


def output_kernel(blocks, o_ref, w_ref, x_ref, max_ref, y_ref, top_ref, part, recv, best, peer_best, send_sem, recv_sem, max_send, max_recv):
    step = pl.program_id(0)
    tp, dp = lax.axis_index("tp"), lax.axis_index("dp")
    other = (1 - tp, dp)

    def exchange(index):
        return pltpu.make_async_remote_copy(
            src_ref=part.at[lax.rem(index, 3)], dst_ref=recv.at[index], send_sem=send_sem.at[lax.rem(index, 3)], recv_sem=recv_sem.at[index], device_id=other, device_id_type=MESH
        )

    def spread(phase, slot, device):
        return pltpu.make_async_remote_copy(
            src_ref=max_ref if phase == 0 else best.at[phase - 1], dst_ref=peer_best.at[slot], send_sem=max_send.at[slot], recv_sem=max_recv.at[slot], device_id=device, device_id_type=MESH
        )

    def phase_copies(phase):
        if phase == 0:
            return [spread(0, 0, other)]
        return [spread(phase, 1 + 3 * (phase - 1) + d, (tp, peer)) for d, peer in enumerate(axis_peers(phase - 1))]

    @pl.when(step == 0)
    def _():
        barrier = pltpu.get_barrier_semaphore()
        peers = [other] + [(tp, peer) for axis in range(3) for peer in axis_peers(axis)]
        for peer in peers:
            pl.semaphore_signal(barrier, inc=1, device_id=peer, device_id_type=MESH)
        pl.semaphore_wait(barrier, len(peers))

    for phase in range(4):
        @pl.when(step == 3 * phase)
        def _():
            for copy in phase_copies(phase):
                copy.start()

        @pl.when(step == 3 * phase + 2)
        def _():
            value = max_ref[...] if phase == 0 else best[phase - 1]
            copies = phase_copies(phase)
            slots = [0] if phase == 0 else [1 + 3 * (phase - 1) + d for d in range(3)]
            for copy, slot in zip(copies, slots):
                copy.wait()
                value = jnp.maximum(value, peer_best[slot])
            if phase < 3:
                best[phase] = value
            else:
                top_ref[...] = value

    def finish(index):
        y_ref[...] = (x_ref[...].astype(f32) + (part[lax.rem(index, 3)] + recv[index])).astype(bf16)

    def multiply():
        part[lax.rem(step, 3)] = jnp.dot(o_ref[...], w_ref[...], preferred_element_type=f32)

    @pl.when(step >= 2)
    def _():
        exchange(step - 2).wait()

    @pl.when(step < 2)
    def _():
        multiply()

    @pl.when((step >= 2) & (step < blocks))
    def _():
        multiply()
        finish(step - 2)

    @pl.when(step >= blocks)
    def _():
        finish(step - 2)

    @pl.when(step < blocks)
    def _():
        exchange(step).start()


def output_projection(o, w_out, x, local_max):
    rows, depth = o.shape
    dim = w_out.shape[1]
    width = 512
    blocks = dim // width
    whole = lambda shape: pl.BlockSpec(shape, lambda j: (0,) * len(shape), pipeline_mode=pl.Buffered(1))
    late = pl.BlockSpec((rows, width), lambda j: (0, jnp.maximum(j - 2, 0)))
    return pl.pallas_call(
        lambda *refs: output_kernel(blocks, *refs),
        grid=(blocks + 2,),
        in_specs=[whole(o.shape), pl.BlockSpec((depth, width), lambda j: (0, jnp.minimum(j, blocks - 1))), late, whole((8, 128))],
        out_specs=[late, whole((8, 128))],
        out_shape=[jax.ShapeDtypeStruct((rows, dim), bf16), jax.ShapeDtypeStruct((8, 128), f32)],
        scratch_shapes=[
            pltpu.VMEM((3, rows, width), f32),
            pltpu.VMEM((blocks, rows, width), f32),
            pltpu.VMEM((3, 8, 128), f32),
            pltpu.VMEM((10, 8, 128), f32),
            pltpu.SemaphoreType.DMA((3,)),
            pltpu.SemaphoreType.DMA((blocks,)),
            pltpu.SemaphoreType.DMA((10,)),
            pltpu.SemaphoreType.DMA((10,)),
        ],
        compiler_params=pltpu.CompilerParams(vmem_limit_bytes=VMEM_MAX, collective_id=0, has_side_effects=True),
        name="output_projection",
    )(o, w_out, x, local_max)


def clip_kernel(top_ref, wqb_ref, wkvb_ref, nqb_ref, nkvb_ref):
    group = pl.program_id(0)
    first = lax.axis_index("tp") * pl.num_programs(0) * GROUP + group * GROUP

    def gains(width, first_dim, second_is_clip):
        column = lax.broadcasted_iota(jnp.int32, (1, GROUP * width), 1)
        best, inner = jnp.full((1, GROUP * width), top_ref[0, first], f32), column
        for i in range(1, GROUP):
            best = jnp.where(column >= i * width, top_ref[0, first + i], best)
            inner = jnp.where(column >= i * width, column - i * width, inner)
        clip = CLIP_TAU / jnp.maximum(CLIP_TAU, best)
        return jnp.where(inner < first_dim, jnp.sqrt(clip), clip if second_is_clip else 1.0)

    nqb_ref[...] = (wqb_ref[...].astype(f32) * gains(QK, NOPE, True)).astype(bf16)
    nkvb_ref[...] = (wkvb_ref[...].astype(f32) * gains(NOPE + VDIM, NOPE, False)).astype(bf16)


def clip(top, wqb, wkvb):
    steps = wqb.shape[1] // (QK * GROUP)
    qspec = pl.BlockSpec((wqb.shape[0], GROUP * QK), lambda g: (0, g))
    kvspec = pl.BlockSpec((wkvb.shape[0], GROUP * (NOPE + VDIM)), lambda g: (0, g))
    return pl.pallas_call(
        clip_kernel,
        grid=(steps,),
        in_specs=[pl.BlockSpec(memory_space=pltpu.SMEM), qspec, kvspec],
        out_specs=[qspec, kvspec],
        out_shape=[jax.ShapeDtypeStruct(wqb.shape, bf16), jax.ShapeDtypeStruct(wkvb.shape, bf16)],
        compiler_params=pltpu.CompilerParams(vmem_limit_bytes=VMEM_MAX),
        name="clip",
    )(top, wqb, wkvb)


def solution(mesh):
    def device_step(hidden, gain_in, gain_q, gain_kv, w_qa, w_kva, w_qb, w_kvb, w_out):
        x = hidden[0]
        tables = rope_tables(x.shape[0])
        qlat, lat, kr = latents(x, gain_in[None], gain_q[None], gain_kv[None], w_qa, w_kva, tables)
        o, local_max = attention(qlat, lat, kr, tables, w_qb, w_kvb)
        y, top = output_projection(o, w_out, x, local_max)
        new_qb, new_kvb = clip(top, w_qb, w_kvb)
        return y[None], top[0, :64], new_qb, new_kvb

    weight_spec = P(None, 'tp')
    return jax.shard_map(device_step, mesh=mesh, in_specs=(P('dp', None, None), P(), P(), P(), P(), P(), weight_spec, weight_spec, P('tp', None)), out_specs=(P('dp', None, None), P(), weight_spec, weight_spec), check_vma=False)
```

```python
import math
import jax
import jax.numpy as jnp
import numpy as np
from jax import lax
from jax.experimental import pallas as pl
from jax.experimental.pallas import tpu as pltpu
from jax.sharding import PartitionSpec as P

NORM_EPS = 1e-6
ROPE_BASE = 50000.0
MSCALE_SQ = (0.1 * math.log(32.0) + 1.0) ** 2
CLIP_TAU = 100.0
NOPE, ROPE, VDIM = 128, 64, 128
QK = NOPE + ROPE
LOGIT_SCALE = QK ** -0.5 * MSCALE_SQ
EXP2_SCALE = LOGIT_SCALE * math.log2(math.e)
GROUP = 4
NEG = -jnp.inf
MESH = pl.DeviceIdType.MESH
VMEM_MAX = 63 * 1024 * 1024
f32, bf16 = jnp.float32, jnp.bfloat16


def rope_tables(seq_len):
    inv_freq = ROPE_BASE ** (-2.0 * np.arange(ROPE // 2) / ROPE)
    angles = np.arange(seq_len)[:, None] * inv_freq[None, :]
    cos, sin = np.cos(angles), np.sin(angles)
    half, rest = np.zeros_like(sin), np.zeros((seq_len, ROPE))
    return np.stack([np.concatenate(t, axis=1) for t in ((cos, cos, rest + 1.0), (-sin, half, rest), (half, sin, rest))]).astype(np.float32)


def turn(tensor, tables):
    return tensor * tables[0] + pltpu.roll(tensor, 96, 1) * tables[1] + pltpu.roll(tensor, 32, 1) * tables[2]


TILE = 256


def latent_kernel(x_hbm, gin_ref, gq_ref, gkv_ref, wqa_hbm, wkva_hbm, tab_ref, qlat_ref, lat_ref, kr_ref, x_ref, n_ref, wq_ref, wkv_ref, wr_ref, full_q, full_kv, rot, scale_ref, x_sem, w_sem, send_sem, recv_sem):
    rows, dim = x_ref.shape
    tp, dp = lax.axis_index("tp"), lax.axis_index("dp")
    other = (1 - tp, dp)
    tiles, parts = wq_ref.shape[0], rows // 128
    rank = lat_ref.shape[1]

    x_copies = [pltpu.make_async_copy(x_hbm.at[pl.ds(r * 128, 128)], x_ref.at[pl.ds(r * 128, 128)], x_sem.at[r]) for r in range(parts)]
    kv_copy = pltpu.make_async_copy(wkva_hbm.at[pl.ds(pl.multiple_of(tp * TILE, TILE), TILE)], wkv_ref, w_sem.at[tiles])
    r_copy = pltpu.make_async_copy(wkva_hbm.at[pl.ds(rank, ROPE)], wr_ref, w_sem.at[tiles + 1])
    q_copies = [pltpu.make_async_copy(wqa_hbm.at[:, pl.ds(pl.multiple_of((tp * tiles + i) * TILE, TILE), TILE)], wq_ref.at[i], w_sem.at[i]) for i in range(tiles)]
    for copy in [*x_copies, *q_copies, kv_copy, r_copy]:
        copy.start()
    barrier = pltpu.get_barrier_semaphore()
    pl.semaphore_signal(barrier, inc=1, device_id=other, device_id_type=MESH)

    def send(ref, index, slot):
        return pltpu.make_async_remote_copy(src_ref=ref.at[index], dst_ref=ref.at[index], send_sem=send_sem.at[slot], recv_sem=recv_sem.at[slot], device_id=other, device_id_type=MESH)

    half = rows // 2

    def measure(part):
        x_copies[2 * part].wait()
        x_copies[2 * part + 1].wait()

        @pl.loop(0, half // 32)
        def _(i):
            here = pl.ds(pl.multiple_of(part * half + i * 32, 32), 32)
            total = jnp.zeros((32, 256), f32)
            for c in range(0, dim, 256):
                v = x_ref[here, c:c + 256].astype(f32)
                total = total + v * v
            scale_ref[here] = jnp.broadcast_to(lax.rsqrt(jnp.sum(total, axis=1, keepdims=True) * (1.0 / dim) + NORM_EPS), (32, 128))

    def normalize(here):
        scale = scale_ref[here, 0:1]
        for c in range(0, dim, 256):
            n_ref[here, c:c + 256] = (x_ref[here, c:c + 256].astype(f32) * scale * gin_ref[:, c:c + 256]).astype(bf16)

    flip = (((1,), (1,)), ((), ()))
    upper, lower = slice(0, half), slice(half, rows)

    measure(0)

    @pl.loop(0, half // 32)
    def _(i):
        normalize(pl.ds(pl.multiple_of(i * 32, 32), 32))

    measure(1)
    q_copies[0].wait()
    q_copies[1].wait()
    for j in range(2):
        full_q[tp * tiles + j, upper] = jnp.dot(n_ref[upper], wq_ref[j], preferred_element_type=f32)
    for r in range(half, rows, 32):
        normalize(slice(r, r + 32))
    pl.semaphore_wait(barrier, 1)
    for j in range(2):
        full_q[tp * tiles + j, lower] = jnp.dot(n_ref[lower], wq_ref[j], preferred_element_type=f32)
    sends = [send(full_q, tp * tiles + j, j) for j in range(2)]
    for copy in sends:
        copy.start()
    q_copies[2].wait()
    for part in (upper, lower):
        full_q[tp * tiles + 2, part] = jnp.dot(n_ref[part], wq_ref[2], preferred_element_type=f32)
    sends.append(send(full_q, tp * tiles + 2, 2))
    sends[2].start()
    kv_copy.wait()
    r_copy.wait()
    for part in (upper, lower):
        full_kv[tp, part] = lax.dot_general(n_ref[part], wkv_ref[...], flip, preferred_element_type=f32)
    sends.append(send(full_kv, tp, tiles))
    sends[3].start()
    quarter = half // 2
    for i in range(2):
        mine = pl.ds(pl.multiple_of(tp * half + i * quarter, quarter), quarter)
        turned = lax.dot_general(n_ref[mine], wr_ref[...], flip, preferred_element_type=f32)
        rot[tp, i * quarter:i * quarter + quarter] = jnp.concatenate([turned, jnp.zeros((quarter, ROPE), f32)], axis=1)
    sends.append(send(rot, tp, tiles + 1))
    sends[4].start()
    for copy in sends[:3]:
        copy.wait()

    @pl.loop(0, rows // 32)
    def _(i):
        here = pl.ds(pl.multiple_of(i * 32, 32), 32)
        pieces = [full_q[j, here] for j in range(2 * tiles)]
        total = sum(a * a for a in pieces)
        scale = lax.rsqrt(jnp.sum(total, axis=1, keepdims=True) * (1.0 / (2 * tiles * TILE)) + NORM_EPS)
        for j, a in enumerate(pieces):
            qlat_ref[here, j * TILE:j * TILE + TILE] = (a * scale * gq_ref[:, j * TILE:j * TILE + TILE]).astype(bf16)

    for copy in sends[3:]:
        copy.wait()
    for r in range(0, rows, 64):
        here = slice(r, r + 64)
        pieces = [full_kv[j, here] for j in range(rank // TILE)]
        total = sum(a * a for a in pieces)
        scale = lax.rsqrt(jnp.sum(total, axis=1, keepdims=True) * (1.0 / rank) + NORM_EPS)
        for j, a in enumerate(pieces):
            lat_ref[here, j * TILE:j * TILE + TILE] = (a * scale * gkv_ref[:, j * TILE:j * TILE + TILE]).astype(bf16)
        key = turn(rot[r // half, r % half:r % half + 64], [tab_ref[i, here] for i in range(3)])
        kr_ref[0, here] = key.astype(bf16)
        kr_ref[1, here] = pltpu.roll(key, 64, 1).astype(bf16)


def latents(x, gin, gq, gkv, wqa, wkva, tables):
    rows, dim = x.shape
    q_rank, rank = wqa.shape[1], gkv.shape[1]
    tiles = q_rank // (2 * TILE)
    vmem, hbm = pl.BlockSpec(memory_space=pltpu.VMEM), pl.BlockSpec(memory_space=pl.ANY)
    return pl.pallas_call(
        latent_kernel,
        in_specs=[hbm, vmem, vmem, vmem, hbm, hbm, vmem],
        out_specs=[vmem, vmem, vmem],
        out_shape=[jax.ShapeDtypeStruct((rows, q_rank), bf16), jax.ShapeDtypeStruct((rows, rank), bf16), jax.ShapeDtypeStruct((2, rows, 128), bf16)],
        scratch_shapes=[
            pltpu.VMEM((rows, dim), bf16),
            pltpu.VMEM((rows, dim), bf16),
            pltpu.VMEM((tiles, dim, TILE), bf16),
            pltpu.VMEM((TILE, dim), bf16),
            pltpu.VMEM((ROPE, dim), bf16),
            pltpu.VMEM((2 * tiles, rows, TILE), f32),
            pltpu.VMEM((rank // TILE, rows, TILE), f32),
            pltpu.VMEM((2, rows // 2, 128), f32),
            pltpu.VMEM((rows, 128), f32),
            pltpu.SemaphoreType.DMA((rows // 128,)),
            pltpu.SemaphoreType.DMA((tiles + 2,)),
            pltpu.SemaphoreType.DMA((tiles + 2,)),
            pltpu.SemaphoreType.DMA((tiles + 2,)),
        ],
        compiler_params=pltpu.CompilerParams(vmem_limit_bytes=VMEM_MAX, collective_id=1, has_side_effects=True),
        name="latents",
    )(x, gin, gq, gkv, wqa, wkva, tables)


BLOCK, CHUNK = 256, 32


def attention_kernel(qlat_ref, lat_ref, kr_ref, tab_ref, wqb_ref, wkvb_ref, o_ref, max_ref, mirror, *scratch):
    step, steps = pl.program_id(0), pl.num_programs(0)
    sets = (scratch[0:3], scratch[3:6])
    raws, probs = scratch[6:10], scratch[10:14]
    heads = (steps - 1) * GROUP
    rows = qlat_ref.shape[0]
    lane = lax.broadcasted_iota(jnp.int32, (rows, 128), 1)

    @pl.when(step == 0)
    def _():
        max_ref[...] = jnp.full((8, 128), NEG, f32)
        for i in range(3):
            mirror[i] = pltpu.roll(tab_ref[i], 64, 1)
        for _, keys, _ in sets:
            for h in range(0, GROUP, 2):
                keys[:, h * 256 + 128:h * 256 + 256] = kr_ref[0]
        for i, prob in enumerate(probs):
            column = 128 + i % 2 * BLOCK
            prob[0:128, column:column + 128] = jnp.zeros((128, 128), bf16)

    def project_q(buffers, n):
        queries = buffers[0]
        chunk = jnp.dot(qlat_ref[...], wqb_ref[:, n * 256:n * 256 + 256], preferred_element_type=f32)
        for i in range(2):
            piece, kind = chunk[:, i * 128:i * 128 + 128], (2 * n + i) % 3
            if kind:
                piece = turn(piece, tab_ref if kind == 1 else mirror)
            queries[:, (2 * n + i) * 128:(2 * n + i) * 128 + 128] = piece.astype(bf16)

    def project_kv(buffers, h):
        _, keys, values = buffers
        chunk = jnp.dot(lat_ref[...], wkvb_ref[:, h * 256:h * 256 + 256], preferred_element_type=f32)
        values[:, h * VDIM:h * VDIM + VDIM] = chunk[:, NOPE:].astype(bf16)
        if h % 2:
            moved = pltpu.roll(chunk[:, :NOPE], 64, 1)
            keys[:, h * 256:h * 256 + 128] = jnp.where(lane >= 64, moved, 0.0).astype(bf16)
            keys[:, h * 256 + 128:h * 256 + 256] = jnp.where(lane < 64, moved.astype(bf16), kr_ref[1])
        else:
            keys[:, h * 256:h * 256 + 128] = chunk[:, :NOPE].astype(bf16)

    def scores(buffers, h):
        queries, keys, _ = buffers
        column = (h // 2) * 384 + (h % 2) * 128
        for b in range(2):
            hi = (b + 1) * BLOCK
            raws[2 * (h % 2) + b][:, :hi] = lax.dot_general(queries[b * BLOCK:hi, column:column + 256], keys[:hi, h * 256:h * 256 + 256], (((1,), (1,)), ((), ())), preferred_element_type=f32)

    def attend(buffers, h):
        values = buffers[2]
        peak = None
        for b in range(2):
            hi = (b + 1) * BLOCK
            raw, prob = raws[2 * (h % 2) + b], probs[2 * (h % 2) + b]
            for r in range(0, BLOCK, CHUNK):
                width = b * BLOCK + (r // 128 + 1) * 128
                tile = raw[r:r + CHUNK, :width]
                keep = lax.broadcasted_iota(jnp.int32, (CHUNK, 128), 0) + r % 128 >= lax.broadcasted_iota(jnp.int32, (CHUNK, 128), 1)
                last = jnp.where(keep, tile[:, width - 128:], NEG)
                tile = last if width == 128 else jnp.concatenate([tile[:, :width - 128], last], axis=1)
                top = jnp.max(tile, axis=1, keepdims=True)
                e = jnp.exp2(tile * EXP2_SCALE - top * EXP2_SCALE)
                prob[r:r + CHUNK, :width] = (e * (1.0 / jnp.sum(e, axis=1, keepdims=True))).astype(bf16)
                peak = top if peak is None else jnp.maximum(peak, top)
            o_ref[b * BLOCK:hi, h * VDIM:h * VDIM + VDIM] = jnp.dot(prob[:, :hi], values[:hi, h * VDIM:h * VDIM + VDIM], preferred_element_type=f32).astype(bf16)
        slot = lax.broadcasted_iota(jnp.int32, (8, 128), 1)
        index = lax.axis_index("tp") * heads + (step - 1) * GROUP + h
        max_ref[...] = jnp.where(slot == index, jnp.max(peak, axis=0, keepdims=True) * LOGIT_SCALE, max_ref[...])

    @pl.when(step == 0)
    def _():
        for n in range(3):
            project_q(sets[0], n)
        for h in range(GROUP):
            project_kv(sets[0], h)
        scores(sets[0], 0)

    for parity in range(2):
        for h in range(GROUP):
            @pl.when((step > 0) & (step < steps - 1) & (lax.rem(step, 2) == parity))
            def _():
                ahead, now = sets[parity], sets[1 - parity]
                if h < GROUP - 1:
                    project_q(ahead, h)
                    scores(now, h + 1)
                else:
                    for i in range(GROUP):
                        project_kv(ahead, i)
                    scores(ahead, 0)
                attend(now, h)

    @pl.when(step == steps - 1)
    def _():
        for h in range(GROUP):
            if h < GROUP - 1:
                scores(sets[1], h + 1)
            attend(sets[1], h)


def attention(qlat, lat, kr, tables, wqb, wkvb):
    rows = qlat.shape[0]
    heads = wqb.shape[1] // QK
    groups = heads // GROUP
    whole = lambda shape: pl.BlockSpec(shape, lambda g: (0,) * len(shape), pipeline_mode=pl.Buffered(1))
    ahead = lambda g: (0, jnp.minimum(g, groups - 1))
    buffers = [pltpu.VMEM((rows, GROUP * QK), bf16), pltpu.VMEM((rows, GROUP * 256), bf16), pltpu.VMEM((rows, GROUP * VDIM), bf16)]
    return pl.pallas_call(
        attention_kernel,
        grid=(groups + 1,),
        in_specs=[whole(qlat.shape), whole(lat.shape), whole(kr.shape), whole(tables.shape), pl.BlockSpec((wqb.shape[0], GROUP * QK), ahead), pl.BlockSpec((wkvb.shape[0], GROUP * (NOPE + VDIM)), ahead)],
        out_specs=[pl.BlockSpec((rows, GROUP * VDIM), lambda g: (0, jnp.maximum(g - 1, 0))), pl.BlockSpec((8, 128), lambda g: (0, 0))],
        out_shape=[jax.ShapeDtypeStruct((rows, heads * VDIM), bf16), jax.ShapeDtypeStruct((8, 128), f32)],
        scratch_shapes=[pltpu.VMEM(tables.shape, f32)] + buffers + buffers + [pltpu.VMEM((BLOCK, (1 + i % 2) * BLOCK), f32) for i in range(4)] + [pltpu.VMEM((BLOCK, (1 + i % 2) * BLOCK), bf16) for i in range(4)],
        compiler_params=pltpu.CompilerParams(vmem_limit_bytes=VMEM_MAX),
        name="attention",
    )(qlat, lat, kr, tables, wqb, wkvb)


def axis_peers(axis):
    dp = lax.axis_index("dp")
    stride = 4 ** axis
    here = lax.rem(dp // stride, 4)
    return [dp + (lax.rem(here + d, 4) - here) * stride for d in (1, 2, 3)]


def output_kernel(blocks, o_ref, w_ref, x_ref, max_ref, y_ref, top_ref, part, recv, best, peer_best, send_sem, recv_sem, max_send, max_recv):
    step = pl.program_id(0)
    tp, dp = lax.axis_index("tp"), lax.axis_index("dp")
    other = (1 - tp, dp)

    def exchange(index):
        return pltpu.make_async_remote_copy(
            src_ref=part.at[lax.rem(index, 3)], dst_ref=recv.at[index], send_sem=send_sem.at[lax.rem(index, 3)], recv_sem=recv_sem.at[index], device_id=other, device_id_type=MESH
        )

    def spread(phase, slot, device):
        return pltpu.make_async_remote_copy(
            src_ref=max_ref if phase == 0 else best.at[phase - 1], dst_ref=peer_best.at[slot], send_sem=max_send.at[slot], recv_sem=max_recv.at[slot], device_id=device, device_id_type=MESH
        )

    def phase_copies(phase):
        if phase == 0:
            return [spread(0, 0, other)]
        return [spread(phase, 1 + 3 * (phase - 1) + d, (tp, peer)) for d, peer in enumerate(axis_peers(phase - 1))]

    @pl.when(step == 0)
    def _():
        barrier = pltpu.get_barrier_semaphore()
        peers = [other] + [(tp, peer) for axis in range(3) for peer in axis_peers(axis)]
        for peer in peers:
            pl.semaphore_signal(barrier, inc=1, device_id=peer, device_id_type=MESH)
        pl.semaphore_wait(barrier, len(peers))

    for phase in range(4):
        @pl.when(step == 3 * phase)
        def _():
            for copy in phase_copies(phase):
                copy.start()

        @pl.when(step == 3 * phase + 2)
        def _():
            value = max_ref[...] if phase == 0 else best[phase - 1]
            copies = phase_copies(phase)
            slots = [0] if phase == 0 else [1 + 3 * (phase - 1) + d for d in range(3)]
            for copy, slot in zip(copies, slots):
                copy.wait()
                value = jnp.maximum(value, peer_best[slot])
            if phase < 3:
                best[phase] = value
            else:
                top_ref[...] = value

    def finish(index):
        y_ref[...] = (x_ref[...].astype(f32) + (part[lax.rem(index, 3)] + recv[index])).astype(bf16)

    def multiply():
        part[lax.rem(step, 3)] = jnp.dot(o_ref[...], w_ref[...], preferred_element_type=f32)
        exchange(step).start()

    @pl.when(step < 2)
    def _():
        multiply()

    @pl.when((step >= 2) & (step < blocks))
    def _():
        exchange(step - 2).wait()
        finish(step - 2)
        multiply()

    @pl.when(step >= blocks)
    def _():
        exchange(step - 2).wait()
        finish(step - 2)


def output_projection(o, w_out, x, local_max):
    rows, depth = o.shape
    dim = w_out.shape[1]
    width = 512
    blocks = dim // width
    whole = lambda shape: pl.BlockSpec(shape, lambda j: (0,) * len(shape), pipeline_mode=pl.Buffered(1))
    late = pl.BlockSpec((rows, width), lambda j: (0, jnp.maximum(j - 2, 0)))
    return pl.pallas_call(
        lambda *refs: output_kernel(blocks, *refs),
        grid=(blocks + 2,),
        in_specs=[whole(o.shape), pl.BlockSpec((depth, width), lambda j: (0, jnp.minimum(j, blocks - 1))), late, whole((8, 128))],
        out_specs=[late, whole((8, 128))],
        out_shape=[jax.ShapeDtypeStruct((rows, dim), bf16), jax.ShapeDtypeStruct((8, 128), f32)],
        scratch_shapes=[
            pltpu.VMEM((3, rows, width), f32),
            pltpu.VMEM((blocks, rows, width), f32),
            pltpu.VMEM((3, 8, 128), f32),
            pltpu.VMEM((10, 8, 128), f32),
            pltpu.SemaphoreType.DMA((3,)),
            pltpu.SemaphoreType.DMA((blocks,)),
            pltpu.SemaphoreType.DMA((10,)),
            pltpu.SemaphoreType.DMA((10,)),
        ],
        compiler_params=pltpu.CompilerParams(vmem_limit_bytes=VMEM_MAX, collective_id=0, has_side_effects=True),
        name="output_projection",
    )(o, w_out, x, local_max)


def clip_kernel(top_ref, wqb_ref, wkvb_ref, nqb_ref, nkvb_ref):
    group = pl.program_id(0)
    first = lax.axis_index("tp") * pl.num_programs(0) * GROUP + group * GROUP

    def gains(width, first_dim, second_is_clip):
        column = lax.broadcasted_iota(jnp.int32, (1, GROUP * width), 1)
        best, inner = jnp.full((1, GROUP * width), top_ref[0, first], f32), column
        for i in range(1, GROUP):
            best = jnp.where(column >= i * width, top_ref[0, first + i], best)
            inner = jnp.where(column >= i * width, column - i * width, inner)
        clip = CLIP_TAU / jnp.maximum(CLIP_TAU, best)
        return jnp.where(inner < first_dim, jnp.sqrt(clip), clip if second_is_clip else 1.0)

    nqb_ref[...] = (wqb_ref[...].astype(f32) * gains(QK, NOPE, True)).astype(bf16)
    nkvb_ref[...] = (wkvb_ref[...].astype(f32) * gains(NOPE + VDIM, NOPE, False)).astype(bf16)


def clip(top, wqb, wkvb):
    steps = wqb.shape[1] // (QK * GROUP)
    qspec = pl.BlockSpec((wqb.shape[0], GROUP * QK), lambda g: (0, g))
    kvspec = pl.BlockSpec((wkvb.shape[0], GROUP * (NOPE + VDIM)), lambda g: (0, g))
    return pl.pallas_call(
        clip_kernel,
        grid=(steps,),
        in_specs=[pl.BlockSpec(memory_space=pltpu.SMEM), qspec, kvspec],
        out_specs=[qspec, kvspec],
        out_shape=[jax.ShapeDtypeStruct(wqb.shape, bf16), jax.ShapeDtypeStruct(wkvb.shape, bf16)],
        compiler_params=pltpu.CompilerParams(vmem_limit_bytes=VMEM_MAX),
        name="clip",
    )(top, wqb, wkvb)


def solution(mesh):
    def device_step(hidden, gain_in, gain_q, gain_kv, w_qa, w_kva, w_qb, w_kvb, w_out):
        x = hidden[0]
        tables = rope_tables(x.shape[0])
        qlat, lat, kr = latents(x, gain_in[None], gain_q[None], gain_kv[None], w_qa, w_kva.T, tables)
        o, local_max = attention(qlat, lat, kr, tables, w_qb, w_kvb)
        y, top = output_projection(o, w_out, x, local_max)
        new_qb, new_kvb = clip(top, w_qb, w_kvb)
        return y[None], top[0, :64], new_qb, new_kvb

    weight_spec = P(None, 'tp')
    return jax.shard_map(device_step, mesh=mesh, in_specs=(P('dp', None, None), P(), P(), P(), P(), P(), weight_spec, weight_spec, P('tp', None)), out_specs=(P('dp', None, None), P(), weight_spec, weight_spec), check_vma=False)
```

```python
import math
import jax
import jax.numpy as jnp
import numpy as np
from jax import lax
from jax.experimental import pallas as pl
from jax.experimental.pallas import tpu as pltpu
from jax.sharding import PartitionSpec as P

NORM_EPS = 1e-6
ROPE_BASE = 50000.0
MSCALE_SQ = (0.1 * math.log(32.0) + 1.0) ** 2
CLIP_TAU = 100.0
NOPE, ROPE, VDIM = 128, 64, 128
QK = NOPE + ROPE
LOGIT_SCALE = QK ** -0.5 * MSCALE_SQ
EXP2_SCALE = LOGIT_SCALE * math.log2(math.e)
GROUP = 4
NEG = -jnp.inf
MESH = pl.DeviceIdType.MESH
MIB = 1024 * 1024
f32, bf16 = jnp.float32, jnp.bfloat16


def rope_tables(seq_len):
    inv_freq = ROPE_BASE ** (-2.0 * np.arange(ROPE // 2) / ROPE)
    angles = np.arange(seq_len)[:, None] * inv_freq[None, :]
    cos, sin = np.cos(angles), np.sin(angles)
    half, rest = np.zeros_like(sin), np.zeros((seq_len, ROPE))
    return np.stack([np.concatenate(t, axis=1) for t in ((cos, cos, rest + 1.0), (-sin, half, rest), (half, sin, rest))]).astype(np.float32)


def in_vmem(array):
    return pltpu.with_memory_space_constraint(array, pltpu.VMEM)


def in_hbm(array):
    return pltpu.with_memory_space_constraint(array, pltpu.HBM)


def turn(tensor, tables):
    return tensor * tables[0] + pltpu.roll(tensor, 96, 1) * tables[1] + pltpu.roll(tensor, 32, 1) * tables[2]


TILE = 256


def latent_kernel(x_hbm, gin_ref, gq_ref, gkv_ref, wqa_hbm, wkva_hbm, tab_ref, qlat_ref, lat_ref, kr_ref, x_ref, n_ref, wq_ref, wkv_ref, wr_ref, full_q, full_kv, rot, scale_ref, x_sem, w_sem, send_sem, recv_sem):
    rows, dim = x_ref.shape
    tp, dp = lax.axis_index("tp"), lax.axis_index("dp")
    other = (1 - tp, dp)
    tiles, parts = wq_ref.shape[0], rows // 128
    rank = lat_ref.shape[1]

    x_copies = [pltpu.make_async_copy(x_hbm.at[pl.ds(r * 128, 128)], x_ref.at[pl.ds(r * 128, 128)], x_sem.at[r]) for r in range(parts)]
    kv_copy = pltpu.make_async_copy(wkva_hbm.at[pl.ds(pl.multiple_of(tp * TILE, TILE), TILE)], wkv_ref, w_sem.at[tiles])
    r_copy = pltpu.make_async_copy(wkva_hbm.at[pl.ds(rank, ROPE)], wr_ref, w_sem.at[tiles + 1])
    q_copies = [pltpu.make_async_copy(wqa_hbm.at[:, pl.ds(pl.multiple_of((tp * tiles + i) * TILE, TILE), TILE)], wq_ref.at[i], w_sem.at[i]) for i in range(tiles)]
    for copy in [*x_copies, *q_copies, kv_copy, r_copy]:
        copy.start()
    barrier = pltpu.get_barrier_semaphore()
    pl.semaphore_signal(barrier, inc=1, device_id=other, device_id_type=MESH)

    def send(ref, index, slot):
        return pltpu.make_async_remote_copy(src_ref=ref.at[index], dst_ref=ref.at[index], send_sem=send_sem.at[slot], recv_sem=recv_sem.at[slot], device_id=other, device_id_type=MESH)

    half = rows // 2

    def measure(part):
        x_copies[2 * part].wait()
        x_copies[2 * part + 1].wait()

        @pl.loop(0, half // 32)
        def _(i):
            here = pl.ds(pl.multiple_of(part * half + i * 32, 32), 32)
            total = jnp.zeros((32, 256), f32)
            for c in range(0, dim, 256):
                v = x_ref[here, c:c + 256].astype(f32)
                total = total + v * v
            scale_ref[here] = jnp.broadcast_to(lax.rsqrt(jnp.sum(total, axis=1, keepdims=True) * (1.0 / dim) + NORM_EPS), (32, 128))

    def normalize(here):
        scale = scale_ref[here, 0:1]
        for c in range(0, dim, 256):
            n_ref[here, c:c + 256] = (x_ref[here, c:c + 256].astype(f32) * scale * gin_ref[:, c:c + 256]).astype(bf16)

    flip = (((1,), (1,)), ((), ()))
    upper, lower = slice(0, half), slice(half, rows)

    measure(0)

    @pl.loop(0, half // 32)
    def _(i):
        normalize(pl.ds(pl.multiple_of(i * 32, 32), 32))

    measure(1)
    q_copies[0].wait()
    q_copies[1].wait()
    for j in range(2):
        full_q[tp * tiles + j, upper] = jnp.dot(n_ref[upper], wq_ref[j], preferred_element_type=f32)
    for r in range(half, rows, 32):
        normalize(slice(r, r + 32))
    pl.semaphore_wait(barrier, 1)
    for j in range(2):
        full_q[tp * tiles + j, lower] = jnp.dot(n_ref[lower], wq_ref[j], preferred_element_type=f32)
    sends = [send(full_q, tp * tiles + j, j) for j in range(2)]
    for copy in sends:
        copy.start()
    q_copies[2].wait()
    for part in (upper, lower):
        full_q[tp * tiles + 2, part] = jnp.dot(n_ref[part], wq_ref[2], preferred_element_type=f32)
    sends.append(send(full_q, tp * tiles + 2, 2))
    sends[2].start()
    kv_copy.wait()
    r_copy.wait()
    for part in (upper, lower):
        full_kv[tp, part] = lax.dot_general(n_ref[part], wkv_ref[...], flip, preferred_element_type=f32)
    sends.append(send(full_kv, tp, tiles))
    sends[3].start()
    quarter = half // 2
    for i in range(2):
        mine = pl.ds(pl.multiple_of(tp * half + i * quarter, quarter), quarter)
        turned = lax.dot_general(n_ref[mine], wr_ref[...], flip, preferred_element_type=f32)
        rot[tp, i * quarter:i * quarter + quarter] = jnp.concatenate([turned, jnp.zeros((quarter, ROPE), f32)], axis=1)
    sends.append(send(rot, tp, tiles + 1))
    sends[4].start()
    for copy in sends[:3]:
        copy.wait()

    @pl.loop(0, rows // 32)
    def _(i):
        here = pl.ds(pl.multiple_of(i * 32, 32), 32)
        pieces = [full_q[j, here] for j in range(2 * tiles)]
        total = sum(a * a for a in pieces)
        scale = lax.rsqrt(jnp.sum(total, axis=1, keepdims=True) * (1.0 / (2 * tiles * TILE)) + NORM_EPS)
        for j, a in enumerate(pieces):
            qlat_ref[here, j * TILE:j * TILE + TILE] = (a * scale * jnp.concatenate([gq_ref[2 * j:2 * j + 1], gq_ref[2 * j + 1:2 * j + 2]], axis=1)).astype(bf16)

    for copy in sends[3:]:
        copy.wait()
    for r in range(0, rows, 64):
        here = slice(r, r + 64)
        pieces = [full_kv[j, here] for j in range(rank // TILE)]
        total = sum(a * a for a in pieces)
        scale = lax.rsqrt(jnp.sum(total, axis=1, keepdims=True) * (1.0 / rank) + NORM_EPS)
        for j, a in enumerate(pieces):
            lat_ref[here, j * TILE:j * TILE + TILE] = (a * scale * gkv_ref[:, j * TILE:j * TILE + TILE]).astype(bf16)
        key = turn(rot[r // half, r % half:r % half + 64], [tab_ref[i, here] for i in range(3)])
        kr_ref[0, here] = key.astype(bf16)
        kr_ref[1, here] = pltpu.roll(key, 64, 1).astype(bf16)


def latents(x, gin, gq, gkv, wqa, wkva, tables):
    rows, dim = x.shape
    q_rank, rank = wqa.shape[1], gkv.shape[1]
    tiles = q_rank // (2 * TILE)
    vmem, hbm = pl.BlockSpec(memory_space=pltpu.VMEM), pl.BlockSpec(memory_space=pltpu.HBM)
    return pl.pallas_call(
        latent_kernel,
        in_specs=[hbm, vmem, vmem, vmem, hbm, hbm, vmem],
        out_specs=[vmem, vmem, vmem],
        out_shape=[pltpu.VMEM((rows, q_rank), bf16), pltpu.VMEM((rows, rank), bf16), pltpu.VMEM((2, rows, 128), bf16)],
        scratch_shapes=[
            pltpu.VMEM((rows, dim), bf16),
            pltpu.VMEM((rows, dim), bf16),
            pltpu.VMEM((tiles, dim, TILE), bf16),
            pltpu.VMEM((TILE, dim), bf16),
            pltpu.VMEM((ROPE, dim), bf16),
            pltpu.VMEM((2 * tiles, rows, TILE), f32),
            pltpu.VMEM((rank // TILE, rows, TILE), f32),
            pltpu.VMEM((2, rows // 2, 128), f32),
            pltpu.VMEM((rows, 128), f32),
            pltpu.SemaphoreType.DMA((rows // 128,)),
            pltpu.SemaphoreType.DMA((tiles + 2,)),
            pltpu.SemaphoreType.DMA((tiles + 2,)),
            pltpu.SemaphoreType.DMA((tiles + 2,)),
        ],
        compiler_params=pltpu.CompilerParams(vmem_limit_bytes=32 * MIB, collective_id=1, has_side_effects=True),
        name="latents",
    )(in_hbm(x), gin, gq, gkv, in_hbm(wqa), in_hbm(wkva), tables)


BLOCK, CHUNK = 256, 32


def attention_kernel(qlat_ref, lat_ref, kr_ref, tab_ref, wqb_hbm, wkvb_ref, o_ref, wqb_ref, max_ref, w_sem, mirror, *scratch):
    step, steps = pl.program_id(0), pl.num_programs(0)
    sets = (scratch[0:3], scratch[3:6])
    raws, probs = scratch[6:10], scratch[10:14]
    heads = o_ref.shape[1] // VDIM
    rows = qlat_ref.shape[0]
    lane = lax.broadcasted_iota(jnp.int32, (rows, 128), 1)

    def fetch(group):
        columns = pl.ds(pl.multiple_of(group * (GROUP * QK), 256), GROUP * QK)
        return pltpu.make_async_copy(wqb_hbm.at[:, columns], wqb_ref.at[:, columns], w_sem.at[group])

    @pl.when(step == 0)
    def _():
        for group in range(heads // GROUP):
            fetch(group).start()

    @pl.when(step < steps - 1)
    def _():
        fetch(step).wait()

    @pl.when(step == 0)
    def _():
        max_ref[...] = jnp.full((8, 128), NEG, f32)
        for i in range(3):
            mirror[i] = pltpu.roll(tab_ref[i], 64, 1)
        for _, keys, _ in sets:
            for h in range(0, GROUP, 2):
                keys[:, h * 256 + 128:h * 256 + 256] = kr_ref[0]
        for i, prob in enumerate(probs):
            column = 128 + i % 2 * BLOCK
            prob[0:128, column:column + 128] = jnp.zeros((128, 128), bf16)

    def project_q(buffers, n):
        queries = buffers[0]
        chunk = jnp.dot(qlat_ref[...], wqb_ref[:, pl.ds(pl.multiple_of(step * (GROUP * QK) + n * 256, 256), 256)], preferred_element_type=f32)
        for i in range(2):
            piece, kind = chunk[:, i * 128:i * 128 + 128], (2 * n + i) % 3
            if kind:
                piece = turn(piece, tab_ref if kind == 1 else mirror)
            queries[:, (2 * n + i) * 128:(2 * n + i) * 128 + 128] = piece.astype(bf16)

    def project_kv(buffers, h):
        _, keys, values = buffers
        chunk = jnp.dot(lat_ref[...], wkvb_ref[:, h * 256:h * 256 + 256], preferred_element_type=f32)
        values[:, h * VDIM:h * VDIM + VDIM] = chunk[:, NOPE:].astype(bf16)
        if h % 2:
            moved = pltpu.roll(chunk[:, :NOPE], 64, 1)
            keys[:, h * 256:h * 256 + 128] = jnp.where(lane >= 64, moved, 0.0).astype(bf16)
            keys[:, h * 256 + 128:h * 256 + 256] = jnp.where(lane < 64, moved.astype(bf16), kr_ref[1])
        else:
            keys[:, h * 256:h * 256 + 128] = chunk[:, :NOPE].astype(bf16)

    def scores(buffers, h):
        queries, keys, _ = buffers
        column = (h // 2) * 384 + (h % 2) * 128
        for b in range(2):
            hi = (b + 1) * BLOCK
            raws[2 * (h % 2) + b][:, :hi] = lax.dot_general(queries[b * BLOCK:hi, column:column + 256], keys[:hi, h * 256:h * 256 + 256], (((1,), (1,)), ((), ())), preferred_element_type=f32)

    def attend(buffers, h):
        values = buffers[2]
        peak = None
        for b in range(2):
            hi = (b + 1) * BLOCK
            raw, prob = raws[2 * (h % 2) + b], probs[2 * (h % 2) + b]
            for r in range(0, BLOCK, CHUNK):
                width = b * BLOCK + (r // 128 + 1) * 128
                tile = raw[r:r + CHUNK, :width]
                keep = lax.broadcasted_iota(jnp.int32, (CHUNK, 128), 0) + r % 128 >= lax.broadcasted_iota(jnp.int32, (CHUNK, 128), 1)
                last = jnp.where(keep, tile[:, width - 128:], NEG)
                tile = last if width == 128 else jnp.concatenate([tile[:, :width - 128], last], axis=1)
                top = jnp.max(tile, axis=1, keepdims=True)
                e = jnp.exp2(tile * EXP2_SCALE - top * EXP2_SCALE)
                prob[r:r + CHUNK, :width] = (e * (1.0 / jnp.sum(e, axis=1, keepdims=True))).astype(bf16)
                peak = top if peak is None else jnp.maximum(peak, top)
            o_ref[b * BLOCK:hi, pl.ds(pl.multiple_of((step - 1) * (GROUP * VDIM) + h * VDIM, VDIM), VDIM)] = jnp.dot(prob[:, :hi], values[:hi, h * VDIM:h * VDIM + VDIM], preferred_element_type=f32).astype(bf16)
        slot = lax.broadcasted_iota(jnp.int32, (8, 128), 1)
        index = lax.axis_index("tp") * heads + (step - 1) * GROUP + h
        max_ref[...] = jnp.where(slot == index, jnp.max(peak, axis=0, keepdims=True) * LOGIT_SCALE, max_ref[...])

    @pl.when(step == 0)
    def _():
        for n in range(3):
            project_q(sets[0], n)
        for h in range(GROUP):
            project_kv(sets[0], h)
        scores(sets[0], 0)

    for parity in range(2):
        for h in range(GROUP):
            @pl.when((step > 0) & (step < steps - 1) & (lax.rem(step, 2) == parity))
            def _():
                ahead, now = sets[parity], sets[1 - parity]
                if h < GROUP - 1:
                    project_q(ahead, h)
                    scores(now, h + 1)
                else:
                    for i in range(GROUP):
                        project_kv(ahead, i)
                    scores(ahead, 0)
                attend(now, h)

    @pl.when(step == steps - 1)
    def _():
        for h in range(GROUP):
            if h < GROUP - 1:
                scores(sets[1], h + 1)
            attend(sets[1], h)


def attention(qlat, lat, kr, tables, wqb, wkvb):
    rows = qlat.shape[0]
    heads = wqb.shape[1] // QK
    groups = heads // GROUP
    vmem, hbm = pl.BlockSpec(memory_space=pltpu.VMEM), pl.BlockSpec(memory_space=pltpu.HBM)
    buffers = [pltpu.VMEM((rows, GROUP * QK), bf16), pltpu.VMEM((rows, GROUP * 256), bf16), pltpu.VMEM((rows, GROUP * VDIM), bf16)]
    return pl.pallas_call(
        attention_kernel,
        grid=(groups + 1,),
        in_specs=[vmem, vmem, vmem, vmem, hbm, pl.BlockSpec((wkvb.shape[0], GROUP * 256), lambda g: (0, jnp.minimum(g, groups - 1)))],
        out_specs=[vmem, vmem, vmem],
        out_shape=[pltpu.VMEM((rows, heads * VDIM), bf16), pltpu.VMEM(wqb.shape, bf16), pltpu.VMEM((8, 128), f32)],
        scratch_shapes=[pltpu.SemaphoreType.DMA((groups,)), pltpu.VMEM(tables.shape, f32)] + buffers + buffers + [pltpu.VMEM((BLOCK, (1 + i % 2) * BLOCK), f32) for i in range(4)] + [pltpu.VMEM((BLOCK, (1 + i % 2) * BLOCK), bf16) for i in range(4)],
        compiler_params=pltpu.CompilerParams(vmem_limit_bytes=15 * MIB),
        name="attention",
    )(in_vmem(qlat), in_vmem(lat), in_vmem(kr), tables, in_hbm(wqb), in_hbm(wkvb))


def axis_peers(axis):
    dp = lax.axis_index("dp")
    stride = 4 ** axis
    here = lax.rem(dp // stride, 4)
    return [dp + (lax.rem(here + d, 4) - here) * stride for d in (1, 2, 3)]


def output_kernel(o_ref, w_hbm, x_hbm, max_ref, y_ref, top_ref, o_buf, w_buf, part, recv, best, peer_best, x_sem, w_sem, send_sem, recv_sem, max_send, max_recv, free_sem):
    slots, rows, width = recv.shape
    blocks = y_ref.shape[1] // width
    tp, dp = lax.axis_index("tp"), lax.axis_index("dp")
    other = (1 - tp, dp)

    def fetch(index):
        slot = lax.rem(index, 2)
        return pltpu.make_async_copy(w_hbm.at[:, pl.ds(pl.multiple_of(index * width, width), width)], w_buf.at[slot], w_sem.at[slot])

    def exchange(index):
        slot, place = lax.rem(index, 3), lax.rem(index, slots)
        return pltpu.make_async_remote_copy(src_ref=part.at[slot], dst_ref=recv.at[place], send_sem=send_sem.at[slot], recv_sem=recv_sem.at[place], device_id=other, device_id_type=MESH)

    def spread(phase, slot, device):
        return pltpu.make_async_remote_copy(
            src_ref=max_ref if phase == 0 else best.at[phase - 1], dst_ref=peer_best.at[slot], send_sem=max_send.at[slot], recv_sem=max_recv.at[slot], device_id=device, device_id_type=MESH
        )

    def phase_slots(phase):
        return [0] if phase == 0 else [1 + 3 * (phase - 1) + d for d in range(3)]

    def phase_copies(phase):
        devices = [other] if phase == 0 else [(tp, peer) for peer in axis_peers(phase - 1)]
        return [spread(phase, slot, device) for slot, device in zip(phase_slots(phase), devices)]

    def finish(index):
        columns = pl.ds(pl.multiple_of(index * width, width), width)
        for r in range(0, rows, 32):
            here = slice(r, r + 32)
            y_ref[here, columns] = (y_ref[here, columns].astype(f32) + (part[lax.rem(index, 3), here] + recv[lax.rem(index, slots), here])).astype(bf16)

    def multiply(index):
        part[lax.rem(index, 3)] = jnp.dot(o_buf[...], w_buf[lax.rem(index, 2)], preferred_element_type=f32)

        @pl.when(index >= slots)
        def _():
            pl.semaphore_wait(free_sem, 1)

        exchange(index).start()

    fetch(0).start()
    fetch(1).start()
    x_copy = pltpu.make_async_copy(x_hbm, y_ref, x_sem)
    x_copy.start()
    barrier = pltpu.get_barrier_semaphore()
    peers = [other] + [(tp, peer) for axis in range(3) for peer in axis_peers(axis)]
    for peer in peers:
        pl.semaphore_signal(barrier, inc=1, device_id=peer, device_id_type=MESH)
    pl.semaphore_wait(barrier, len(peers))
    for copy in phase_copies(0):
        copy.start()

    @pl.loop(0, rows // 32)
    def _(i):
        here = pl.ds(pl.multiple_of(i * 32, 32), 32)
        o_buf[here] = o_ref[here]

    @pl.loop(0, 2)
    def _(index):
        fetch(index).wait()
        multiply(index)
        fetch(index + 2).start()

    x_copy.wait()

    @pl.loop(2, blocks)
    def _(index):
        for phase in range(4):
            @pl.when(index == 3 * phase + 2)
            def _():
                value = max_ref[...] if phase == 0 else best[phase - 1]
                for copy, slot in zip(phase_copies(phase), phase_slots(phase)):
                    copy.wait()
                    value = jnp.maximum(value, peer_best[slot])
                if phase < 3:
                    best[phase] = value
                else:
                    top_ref[...] = value

            if phase:
                @pl.when(index == 3 * phase)
                def _():
                    for copy in phase_copies(phase):
                        copy.start()

        fetch(index).wait()
        exchange(index - 2).wait()
        finish(index - 2)
        multiply(index)

        @pl.when(index - 2 < blocks - slots)
        def _():
            pl.semaphore_signal(free_sem, inc=1, device_id=other, device_id_type=MESH)

        @pl.when(index + 2 < blocks)
        def _():
            fetch(index + 2).start()

    for index in (blocks - 2, blocks - 1):
        exchange(index).wait()
        finish(index)


def output_projection(o, w_out, x, local_max):
    rows, depth = o.shape
    dim = w_out.shape[1]
    width = 512
    slots = 4
    vmem, hbm = pl.BlockSpec(memory_space=pltpu.VMEM), pl.BlockSpec(memory_space=pltpu.HBM)
    return pl.pallas_call(
        output_kernel,
        in_specs=[vmem, hbm, hbm, vmem],
        out_specs=[vmem, vmem],
        out_shape=[pltpu.VMEM((rows, dim), bf16), jax.ShapeDtypeStruct((8, 128), f32)],
        scratch_shapes=[
            pltpu.VMEM(o.shape, bf16),
            pltpu.VMEM((2, depth, width), bf16),
            pltpu.VMEM((3, rows, width), f32),
            pltpu.VMEM((slots, rows, width), f32),
            pltpu.VMEM((3, 8, 128), f32),
            pltpu.VMEM((10, 8, 128), f32),
            pltpu.SemaphoreType.DMA,
            pltpu.SemaphoreType.DMA((2,)),
            pltpu.SemaphoreType.DMA((3,)),
            pltpu.SemaphoreType.DMA((slots,)),
            pltpu.SemaphoreType.DMA((10,)),
            pltpu.SemaphoreType.DMA((10,)),
            pltpu.SemaphoreType.REGULAR,
        ],
        compiler_params=pltpu.CompilerParams(vmem_limit_bytes=20 * MIB, collective_id=0, has_side_effects=True),
        name="output_projection",
    )(in_vmem(o), in_hbm(w_out), in_hbm(x), in_vmem(local_max))


def clip_kernel(top_ref, wqb_ref, wkvb_ref, y_ref, nqb_ref, nkvb_ref, out_hbm, max_ref, y_sem):
    group, groups = pl.program_id(0), pl.num_programs(0)
    first = lax.axis_index("tp") * groups * GROUP + group * GROUP
    y_copy = pltpu.make_async_copy(y_ref, out_hbm, y_sem)

    @pl.when(group == 0)
    def _():
        y_copy.start()
        for i in range(max_ref.shape[0]):
            max_ref[i] = top_ref[0, i]

    def gains(width, first_dim, second_is_clip):
        column = lax.broadcasted_iota(jnp.int32, (1, GROUP * width), 1)
        best, inner = jnp.full((1, GROUP * width), top_ref[0, first], f32), column
        for i in range(1, GROUP):
            best = jnp.where(column >= i * width, top_ref[0, first + i], best)
            inner = jnp.where(column >= i * width, column - i * width, inner)
        clip = CLIP_TAU / jnp.maximum(CLIP_TAU, best)
        return jnp.where(inner < first_dim, jnp.sqrt(clip), clip if second_is_clip else 1.0)

    for src, dst, width, first_dim, second_is_clip in ((wqb_ref, nqb_ref, QK, NOPE, True), (wkvb_ref, nkvb_ref, NOPE + VDIM, NOPE, False)):
        gain = gains(width, first_dim, second_is_clip)
        columns = pl.ds(pl.multiple_of(group * GROUP * width, 256), GROUP * width) if second_is_clip else slice(None)

        @pl.loop(0, src.shape[0] // 256)
        def _(i):
            here = pl.ds(pl.multiple_of(i * 256, 256), 256)
            dst[here] = (src[here, columns].astype(f32) * gain).astype(bf16)

    @pl.when(group == groups - 1)
    def _():
        y_copy.wait()


def clip(top, wqb, wkvb, y, all_heads):
    steps = wqb.shape[1] // (QK * GROUP)
    vmem = pl.BlockSpec(memory_space=pltpu.VMEM)
    qspec = pl.BlockSpec((wqb.shape[0], GROUP * QK), lambda g: (0, g))
    kvspec = pl.BlockSpec((wkvb.shape[0], GROUP * (NOPE + VDIM)), lambda g: (0, g))
    return pl.pallas_call(
        clip_kernel,
        grid=(steps,),
        in_specs=[pl.BlockSpec(memory_space=pltpu.SMEM), vmem, kvspec, vmem],
        out_specs=[qspec, kvspec, pl.BlockSpec(memory_space=pltpu.HBM), pl.BlockSpec(memory_space=pltpu.SMEM)],
        out_shape=[jax.ShapeDtypeStruct(wqb.shape, bf16), jax.ShapeDtypeStruct(wkvb.shape, bf16), jax.ShapeDtypeStruct(y.shape, bf16), jax.ShapeDtypeStruct((all_heads,), f32)],
        scratch_shapes=[pltpu.SemaphoreType.DMA],
        compiler_params=pltpu.CompilerParams(vmem_limit_bytes=10 * MIB),
        name="clip",
    )(top, in_vmem(wqb), in_hbm(wkvb), in_vmem(y))


def solution(mesh):
    def device_step(hidden, gain_in, gain_q, gain_kv, w_qa, w_kva, w_qb, w_kvb, w_out):
        x = hidden[0]
        tables = rope_tables(x.shape[0])
        qlat, lat, kr = latents(x, gain_in[None], gain_q.reshape(-1, 128), gain_kv[None], w_qa, w_kva.T, tables)
        o, keep_qb, local_max = attention(qlat, lat, kr, tables, w_qb, w_kvb)
        y, top = output_projection(o, w_out, x, local_max)
        new_qb, new_kvb, out, logit_max = clip(top, keep_qb, w_kvb, y, mesh.shape["tp"] * o.shape[1] // VDIM)
        return out[None], logit_max, new_qb, new_kvb

    weight_spec = P(None, 'tp')
    return jax.shard_map(device_step, mesh=mesh, in_specs=(P('dp', None, None), P(), P(), P(), P(), P(), weight_spec, weight_spec, P('tp', None)), out_specs=(P('dp', None, None), P(), weight_spec, weight_spec), check_vma=False)
```

```python
import math
import jax
import jax.numpy as jnp
import numpy as np
from jax import lax
from jax.experimental import pallas as pl
from jax.experimental.pallas import tpu as pltpu
from jax.sharding import PartitionSpec as P

NORM_EPS = 1e-6
ROPE_BASE = 50000.0
MSCALE_SQ = (0.1 * math.log(32.0) + 1.0) ** 2
CLIP_TAU = 100.0
NOPE, ROPE, VDIM = 128, 64, 128
QK = NOPE + ROPE
LOGIT_SCALE = QK ** -0.5 * MSCALE_SQ
EXP2_SCALE = LOGIT_SCALE * math.log2(math.e)
GROUP = 4
NEG = -jnp.inf
MESH = pl.DeviceIdType.MESH
MIB = 1024 * 1024
f32, bf16 = jnp.float32, jnp.bfloat16


def rope_tables(seq_len):
    inv_freq = ROPE_BASE ** (-2.0 * np.arange(ROPE // 2) / ROPE)
    angles = np.arange(seq_len)[:, None] * inv_freq[None, :]
    cos, sin = np.cos(angles), np.sin(angles)
    half, rest = np.zeros_like(sin), np.zeros((seq_len, ROPE))
    return np.stack([np.concatenate(t, axis=1) for t in ((cos, cos, rest + 1.0), (-sin, half, rest), (half, sin, rest))]).astype(np.float32)


def in_vmem(array):
    return pltpu.with_memory_space_constraint(array, pltpu.VMEM)


def in_hbm(array):
    return pltpu.with_memory_space_constraint(array, pltpu.HBM)


def turn(tensor, tables):
    return tensor * tables[0] + pltpu.roll(tensor, 96, 1) * tables[1] + pltpu.roll(tensor, 32, 1) * tables[2]


TILE = 256


def latent_kernel(x_hbm, gin_hbm, gq_hbm, gkv_hbm, wqa_hbm, wkva_hbm, tab_hbm, wqb_hbm, qlat_ref, lat_ref, kr_ref, tab_ref, wqb_ref, gin_ref, gq_ref, gkv_ref, g_sem, x_ref, n_ref, wq_ref, wkv_ref, wr_ref, full_q, full_kv, rot, scale_ref, x_sem, w_sem, send_sem, recv_sem):
    rows, dim = x_ref.shape
    tp, dp = lax.axis_index("tp"), lax.axis_index("dp")
    other = (1 - tp, dp)
    tiles, parts = wq_ref.shape[0], rows // 128
    rank = lat_ref.shape[1]

    x_copies = [pltpu.make_async_copy(x_hbm.at[pl.ds(r * 128, 128)], x_ref.at[pl.ds(r * 128, 128)], x_sem.at[r]) for r in range(parts)]
    kv_copy = pltpu.make_async_copy(wkva_hbm.at[pl.ds(pl.multiple_of(tp * TILE, TILE), TILE)], wkv_ref, w_sem.at[tiles])
    r_copy = pltpu.make_async_copy(wkva_hbm.at[pl.ds(rank, ROPE)], wr_ref, w_sem.at[tiles + 1])
    q_copies = [pltpu.make_async_copy(wqa_hbm.at[:, pl.ds(pl.multiple_of((tp * tiles + i) * TILE, TILE), TILE)], wq_ref.at[i], w_sem.at[i]) for i in range(tiles)]
    small = [pltpu.make_async_copy(src, dst, g_sem.at[i]) for i, (src, dst) in enumerate(((gin_hbm, gin_ref), (gq_hbm, gq_ref), (gkv_hbm, gkv_ref), (tab_hbm, tab_ref), (wqb_hbm, wqb_ref)))]
    for copy in [*x_copies, *small[:3]]:
        copy.start()
    barrier = pltpu.get_barrier_semaphore()
    pl.semaphore_signal(barrier, inc=1, device_id=other, device_id_type=MESH)

    def send(ref, index, slot):
        return pltpu.make_async_remote_copy(src_ref=ref.at[index], dst_ref=ref.at[index], send_sem=send_sem.at[slot], recv_sem=recv_sem.at[slot], device_id=other, device_id_type=MESH)

    half = rows // 2

    def measure(part):
        x_copies[2 * part].wait()
        x_copies[2 * part + 1].wait()

        @pl.loop(0, half // 32)
        def _(i):
            here = pl.ds(pl.multiple_of(part * half + i * 32, 32), 32)
            total = jnp.zeros((32, 256), f32)
            for c in range(0, dim, 256):
                v = x_ref[here, c:c + 256].astype(f32)
                total = total + v * v
            scale_ref[here] = jnp.broadcast_to(lax.rsqrt(jnp.sum(total, axis=1, keepdims=True) * (1.0 / dim) + NORM_EPS), (32, 128))

    def normalize(here):
        scale = scale_ref[here, 0:1]
        for c in range(0, dim, 256):
            n_ref[here, c:c + 256] = (x_ref[here, c:c + 256].astype(f32) * scale * gin_ref[:, c:c + 256]).astype(bf16)

    flip = (((1,), (1,)), ((), ()))
    upper, lower = slice(0, half), slice(half, rows)

    measure(0)
    q_copies[0].start()
    q_copies[1].start()
    for copy in small[:3]:
        copy.wait()

    @pl.loop(0, half // 32)
    def _(i):
        normalize(pl.ds(pl.multiple_of(i * 32, 32), 32))

    measure(1)
    for copy in [q_copies[2], kv_copy, r_copy, small[3]]:
        copy.start()
    q_copies[0].wait()
    q_copies[1].wait()
    for j in range(2):
        full_q[tp * tiles + j, upper] = jnp.dot(n_ref[upper], wq_ref[j], preferred_element_type=f32)
    for r in range(half, rows, 32):
        normalize(slice(r, r + 32))
    pl.semaphore_wait(barrier, 1)
    for j in range(2):
        full_q[tp * tiles + j, lower] = jnp.dot(n_ref[lower], wq_ref[j], preferred_element_type=f32)
    sends = [send(full_q, tp * tiles + j, j) for j in range(2)]
    for copy in sends:
        copy.start()
    small[4].start()
    q_copies[2].wait()
    for part in (upper, lower):
        full_q[tp * tiles + 2, part] = jnp.dot(n_ref[part], wq_ref[2], preferred_element_type=f32)
    sends.append(send(full_q, tp * tiles + 2, 2))
    sends[2].start()
    kv_copy.wait()
    r_copy.wait()
    for part in (upper, lower):
        full_kv[tp, part] = lax.dot_general(n_ref[part], wkv_ref[...], flip, preferred_element_type=f32)
    sends.append(send(full_kv, tp, tiles))
    sends[3].start()
    quarter = half // 2
    for i in range(2):
        mine = pl.ds(pl.multiple_of(tp * half + i * quarter, quarter), quarter)
        turned = lax.dot_general(n_ref[mine], wr_ref[...], flip, preferred_element_type=f32)
        rot[tp, i * quarter:i * quarter + quarter] = jnp.concatenate([turned, jnp.zeros((quarter, ROPE), f32)], axis=1)
    sends.append(send(rot, tp, tiles + 1))
    sends[4].start()
    for copy in sends[:3]:
        copy.wait()

    @pl.loop(0, rows // 32)
    def _(i):
        here = pl.ds(pl.multiple_of(i * 32, 32), 32)
        pieces = [full_q[j, here] for j in range(2 * tiles)]
        total = sum(a * a for a in pieces)
        scale = lax.rsqrt(jnp.sum(total, axis=1, keepdims=True) * (1.0 / (2 * tiles * TILE)) + NORM_EPS)
        for j, a in enumerate(pieces):
            qlat_ref[here, j * TILE:j * TILE + TILE] = (a * scale * jnp.concatenate([gq_ref[2 * j:2 * j + 1], gq_ref[2 * j + 1:2 * j + 2]], axis=1)).astype(bf16)

    for copy in [*sends[3:], small[3]]:
        copy.wait()
    for r in range(0, rows, 64):
        here = slice(r, r + 64)
        pieces = [full_kv[j, here] for j in range(rank // TILE)]
        total = sum(a * a for a in pieces)
        scale = lax.rsqrt(jnp.sum(total, axis=1, keepdims=True) * (1.0 / rank) + NORM_EPS)
        for j, a in enumerate(pieces):
            lat_ref[here, j * TILE:j * TILE + TILE] = (a * scale * gkv_ref[:, j * TILE:j * TILE + TILE]).astype(bf16)
        key = turn(rot[r // half, r % half:r % half + 64], [tab_ref[i, here] for i in range(3)])
        kr_ref[0, here] = key.astype(bf16)
        kr_ref[1, here] = pltpu.roll(key, 64, 1).astype(bf16)
    small[4].wait()


def latents(x, gin, gq, gkv, wqa, wkva, tables, wqb):
    rows, dim = x.shape
    q_rank, rank = wqa.shape[1], gkv.shape[1]
    tiles = q_rank // (2 * TILE)
    vmem, hbm = pl.BlockSpec(memory_space=pltpu.VMEM), pl.BlockSpec(memory_space=pltpu.HBM)
    return pl.pallas_call(
        latent_kernel,
        in_specs=[hbm] * 8,
        out_specs=[vmem] * 5,
        out_shape=[pltpu.VMEM((rows, q_rank), bf16), pltpu.VMEM((rows, rank), bf16), pltpu.VMEM((2, rows, 128), bf16), pltpu.VMEM(tables.shape, f32), pltpu.VMEM(wqb.shape, bf16)],
        scratch_shapes=[
            pltpu.VMEM(gin.shape, f32),
            pltpu.VMEM(gq.shape, f32),
            pltpu.VMEM(gkv.shape, f32),
            pltpu.SemaphoreType.DMA((5,)),
            pltpu.VMEM((rows, dim), bf16),
            pltpu.VMEM((rows, dim), bf16),
            pltpu.VMEM((tiles, dim, TILE), bf16),
            pltpu.VMEM((TILE, dim), bf16),
            pltpu.VMEM((ROPE, dim), bf16),
            pltpu.VMEM((2 * tiles, rows, TILE), f32),
            pltpu.VMEM((rank // TILE, rows, TILE), f32),
            pltpu.VMEM((2, rows // 2, 128), f32),
            pltpu.VMEM((rows, 128), f32),
            pltpu.SemaphoreType.DMA((rows // 128,)),
            pltpu.SemaphoreType.DMA((tiles + 2,)),
            pltpu.SemaphoreType.DMA((tiles + 2,)),
            pltpu.SemaphoreType.DMA((tiles + 2,)),
        ],
        compiler_params=pltpu.CompilerParams(vmem_limit_bytes=32 * MIB, collective_id=1, has_side_effects=True),
        name="latents",
    )(*(in_hbm(a) for a in (x, gin, gq, gkv, wqa, wkva, tables, wqb)))


BLOCK, CHUNK, WIDTH = 256, 32, 512


def attention_kernel(qlat_ref, lat_ref, kr_ref, tab_ref, wqb_ref, wkvb_ref, wout_hbm, o_ref, max_ref, head_ref, w_sem, mirror, *scratch):
    step, steps = pl.program_id(0), pl.num_programs(0)
    sets = (scratch[0:3], scratch[3:6])
    raws, probs = scratch[6:10], scratch[10:14]
    heads = o_ref.shape[1] // VDIM
    rows = qlat_ref.shape[0]
    lane = lax.broadcasted_iota(jnp.int32, (rows, 128), 1)

    head_copy = pltpu.make_async_copy(wout_hbm.at[:, pl.ds(0, head_ref.shape[1])], head_ref, w_sem)

    @pl.when(step == 1)
    def _():
        head_copy.start()

    @pl.when(step == steps - 1)
    def _():
        head_copy.wait()

    @pl.when(step == 0)
    def _():
        max_ref[...] = jnp.full((8, 128), NEG, f32)
        for i in range(3):
            mirror[i] = pltpu.roll(tab_ref[i], 64, 1)
        for _, keys, _ in sets:
            for h in range(0, GROUP, 2):
                keys[:, h * 256 + 128:h * 256 + 256] = kr_ref[0]
        for i, prob in enumerate(probs):
            column = 128 + i % 2 * BLOCK
            prob[0:128, column:column + 128] = jnp.zeros((128, 128), bf16)

    def project_q(buffers, n):
        queries = buffers[0]
        chunk = jnp.dot(qlat_ref[...], wqb_ref[:, pl.ds(pl.multiple_of(step * (GROUP * QK) + n * 256, 256), 256)], preferred_element_type=f32)
        for i in range(2):
            piece, kind = chunk[:, i * 128:i * 128 + 128], (2 * n + i) % 3
            if kind:
                piece = turn(piece, tab_ref if kind == 1 else mirror)
            queries[:, (2 * n + i) * 128:(2 * n + i) * 128 + 128] = piece.astype(bf16)

    def project_kv(buffers, h):
        _, keys, values = buffers
        chunk = jnp.dot(lat_ref[...], wkvb_ref[:, h * 256:h * 256 + 256], preferred_element_type=f32)
        values[:, h * VDIM:h * VDIM + VDIM] = chunk[:, NOPE:].astype(bf16)
        if h % 2:
            moved = pltpu.roll(chunk[:, :NOPE], 64, 1)
            keys[:, h * 256:h * 256 + 128] = jnp.where(lane >= 64, moved, 0.0).astype(bf16)
            keys[:, h * 256 + 128:h * 256 + 256] = jnp.where(lane < 64, moved.astype(bf16), kr_ref[1])
        else:
            keys[:, h * 256:h * 256 + 128] = chunk[:, :NOPE].astype(bf16)

    def scores(buffers, h):
        queries, keys, _ = buffers
        column = (h // 2) * 384 + (h % 2) * 128
        for b in range(2):
            hi = (b + 1) * BLOCK
            raws[2 * (h % 2) + b][:, :hi] = lax.dot_general(queries[b * BLOCK:hi, column:column + 256], keys[:hi, h * 256:h * 256 + 256], (((1,), (1,)), ((), ())), preferred_element_type=f32)

    def attend(buffers, h):
        values = buffers[2]
        peak = None
        for b in range(2):
            hi = (b + 1) * BLOCK
            raw, prob = raws[2 * (h % 2) + b], probs[2 * (h % 2) + b]
            for r in range(0, BLOCK, CHUNK):
                width = b * BLOCK + (r // 128 + 1) * 128
                tile = raw[r:r + CHUNK, :width]
                keep = lax.broadcasted_iota(jnp.int32, (CHUNK, 128), 0) + r % 128 >= lax.broadcasted_iota(jnp.int32, (CHUNK, 128), 1)
                last = jnp.where(keep, tile[:, width - 128:], NEG)
                tile = last if width == 128 else jnp.concatenate([tile[:, :width - 128], last], axis=1)
                top = jnp.max(tile, axis=1, keepdims=True)
                e = jnp.exp2(tile * EXP2_SCALE - top * EXP2_SCALE)
                prob[r:r + CHUNK, :width] = (e * (1.0 / jnp.sum(e, axis=1, keepdims=True))).astype(bf16)
                peak = top if peak is None else jnp.maximum(peak, top)
            o_ref[b * BLOCK:hi, pl.ds(pl.multiple_of((step - 1) * (GROUP * VDIM) + h * VDIM, VDIM), VDIM)] = jnp.dot(prob[:, :hi], values[:hi, h * VDIM:h * VDIM + VDIM], preferred_element_type=f32).astype(bf16)
        slot = lax.broadcasted_iota(jnp.int32, (8, 128), 1)
        index = lax.axis_index("tp") * heads + (step - 1) * GROUP + h
        max_ref[...] = jnp.where(slot == index, jnp.max(peak, axis=0, keepdims=True) * LOGIT_SCALE, max_ref[...])

    @pl.when(step == 0)
    def _():
        for n in range(3):
            project_q(sets[0], n)
        for h in range(GROUP):
            project_kv(sets[0], h)
        scores(sets[0], 0)

    for parity in range(2):
        for h in range(GROUP):
            @pl.when((step > 0) & (step < steps - 1) & (lax.rem(step, 2) == parity))
            def _():
                ahead, now = sets[parity], sets[1 - parity]
                if h < GROUP - 1:
                    project_q(ahead, h)
                    scores(now, h + 1)
                else:
                    for i in range(GROUP):
                        project_kv(ahead, i)
                    scores(ahead, 0)
                attend(now, h)

    @pl.when(step == steps - 1)
    def _():
        for h in range(GROUP):
            if h < GROUP - 1:
                scores(sets[1], h + 1)
            attend(sets[1], h)


def attention(qlat, lat, kr, tables, wqb, wkvb, w_out):
    rows = qlat.shape[0]
    heads = wqb.shape[1] // QK
    groups = heads // GROUP
    vmem, hbm = pl.BlockSpec(memory_space=pltpu.VMEM), pl.BlockSpec(memory_space=pltpu.HBM)
    buffers = [pltpu.VMEM((rows, GROUP * QK), bf16), pltpu.VMEM((rows, GROUP * 256), bf16), pltpu.VMEM((rows, GROUP * VDIM), bf16)]
    return pl.pallas_call(
        attention_kernel,
        grid=(groups + 1,),
        in_specs=[vmem, vmem, vmem, vmem, vmem, pl.BlockSpec((wkvb.shape[0], GROUP * 256), lambda g: (0, jnp.minimum(g, groups - 1))), hbm],
        out_specs=[vmem, vmem, vmem],
        out_shape=[pltpu.VMEM((rows, heads * VDIM), bf16), pltpu.VMEM((8, 128), f32), pltpu.VMEM((w_out.shape[0], WIDTH), bf16)],
        scratch_shapes=[pltpu.SemaphoreType.DMA, pltpu.VMEM(tables.shape, f32)] + buffers + buffers + [pltpu.VMEM((BLOCK, (1 + i % 2) * BLOCK), f32) for i in range(4)] + [pltpu.VMEM((BLOCK, (1 + i % 2) * BLOCK), bf16) for i in range(4)],
        compiler_params=pltpu.CompilerParams(vmem_limit_bytes=15 * MIB),
        name="attention",
    )(in_vmem(qlat), in_vmem(lat), in_vmem(kr), in_vmem(tables), in_vmem(wqb), in_hbm(wkvb), in_hbm(w_out))


def axis_peers(axis):
    dp = lax.axis_index("dp")
    stride = 4 ** axis
    here = lax.rem(dp // stride, 4)
    return [dp + (lax.rem(here + d, 4) - here) * stride for d in (1, 2, 3)]


def output_kernel(o_ref, head_ref, w_hbm, x_hbm, max_ref, y_ref, top_ref, o_buf, w_buf, part, recv, best, peer_best, x_sem, w_sem, send_sem, recv_sem, max_send, max_recv, free_sem):
    slots, rows, width = recv.shape
    blocks = y_ref.shape[1] // width
    tp, dp = lax.axis_index("tp"), lax.axis_index("dp")
    other = (1 - tp, dp)

    def fetch(index):
        slot = lax.rem(index, 2)
        return pltpu.make_async_copy(w_hbm.at[:, pl.ds(pl.multiple_of(index * width, width), width)], w_buf.at[slot], w_sem.at[slot])

    def exchange(index):
        slot, place = lax.rem(index, 3), lax.rem(index, slots)
        return pltpu.make_async_remote_copy(src_ref=part.at[slot], dst_ref=recv.at[place], send_sem=send_sem.at[slot], recv_sem=recv_sem.at[place], device_id=other, device_id_type=MESH)

    def spread(phase, slot, device):
        return pltpu.make_async_remote_copy(
            src_ref=max_ref if phase == 0 else best.at[phase - 1], dst_ref=peer_best.at[slot], send_sem=max_send.at[slot], recv_sem=max_recv.at[slot], device_id=device, device_id_type=MESH
        )

    def phase_slots(phase):
        return [0] if phase == 0 else [1 + 3 * (phase - 1) + d for d in range(3)]

    def phase_copies(phase):
        devices = [other] if phase == 0 else [(tp, peer) for peer in axis_peers(phase - 1)]
        return [spread(phase, slot, device) for slot, device in zip(phase_slots(phase), devices)]

    def finish(index):
        columns = pl.ds(pl.multiple_of(index * width, width), width)
        for r in range(0, rows, 32):
            here = slice(r, r + 32)
            y_ref[here, columns] = (y_ref[here, columns].astype(f32) + (part[lax.rem(index, 3), here] + recv[lax.rem(index, slots), here])).astype(bf16)

    fetch(1).start()
    x_copy = pltpu.make_async_copy(x_hbm, y_ref, x_sem)
    x_copy.start()
    barrier = pltpu.get_barrier_semaphore()
    peers = [other] + [(tp, peer) for axis in range(3) for peer in axis_peers(axis)]
    for peer in peers:
        pl.semaphore_signal(barrier, inc=1, device_id=peer, device_id_type=MESH)
    pl.semaphore_wait(barrier, len(peers))
    for copy in phase_copies(0):
        copy.start()

    @pl.loop(0, rows // 32)
    def _(i):
        here = pl.ds(pl.multiple_of(i * 32, 32), 32)
        o_buf[here] = o_ref[here]

    for index in range(2):
        if index:
            fetch(index).wait()
        else:
            fetch(2).start()
        part[index] = jnp.dot(o_buf[...], w_buf[1] if index else head_ref[...], preferred_element_type=f32)
        exchange(index).start()
    fetch(3).start()
    x_copy.wait()

    @pl.loop(2, blocks)
    def _(index):
        for phase in range(4):
            @pl.when(index == 3 * phase + 2)
            def _():
                value = max_ref[...] if phase == 0 else best[phase - 1]
                for copy, slot in zip(phase_copies(phase), phase_slots(phase)):
                    copy.wait()
                    value = jnp.maximum(value, peer_best[slot])
                if phase < 3:
                    best[phase] = value
                else:
                    top_ref[...] = value

            if phase:
                @pl.when(index == 3 * phase)
                def _():
                    for copy in phase_copies(phase):
                        copy.start()

        fetch(index).wait()
        exchange(index - 2).wait()
        finish(index - 2)
        part[lax.rem(index, 3)] = jnp.dot(o_buf[...], w_buf[lax.rem(index, 2)], preferred_element_type=f32)

        @pl.when(index >= slots)
        def _():
            pl.semaphore_wait(free_sem, 1)

        exchange(index).start()

        @pl.when(index - 2 < blocks - slots)
        def _():
            pl.semaphore_signal(free_sem, inc=1, device_id=other, device_id_type=MESH)

        @pl.when(index + 2 < blocks)
        def _():
            fetch(index + 2).start()

    for index in (blocks - 2, blocks - 1):
        exchange(index).wait()
        finish(index)


def output_projection(o, head, w_out, x, local_max):
    rows, depth = o.shape
    dim = w_out.shape[1]
    width = WIDTH
    slots = 4
    vmem, hbm = pl.BlockSpec(memory_space=pltpu.VMEM), pl.BlockSpec(memory_space=pltpu.HBM)
    return pl.pallas_call(
        output_kernel,
        in_specs=[vmem, vmem, hbm, hbm, vmem],
        out_specs=[vmem, vmem],
        out_shape=[pltpu.VMEM((rows, dim), bf16), jax.ShapeDtypeStruct((8, 128), f32)],
        scratch_shapes=[
            pltpu.VMEM(o.shape, bf16),
            pltpu.VMEM((2, depth, width), bf16),
            pltpu.VMEM((3, rows, width), f32),
            pltpu.VMEM((slots, rows, width), f32),
            pltpu.VMEM((3, 8, 128), f32),
            pltpu.VMEM((10, 8, 128), f32),
            pltpu.SemaphoreType.DMA,
            pltpu.SemaphoreType.DMA((2,)),
            pltpu.SemaphoreType.DMA((3,)),
            pltpu.SemaphoreType.DMA((slots,)),
            pltpu.SemaphoreType.DMA((10,)),
            pltpu.SemaphoreType.DMA((10,)),
            pltpu.SemaphoreType.REGULAR,
        ],
        compiler_params=pltpu.CompilerParams(vmem_limit_bytes=20 * MIB, collective_id=0, has_side_effects=True),
        name="output_projection",
    )(in_vmem(o), in_vmem(head), in_hbm(w_out), in_hbm(x), in_vmem(local_max))


def clip_kernel(top_ref, wqb_ref, wkvb_ref, y_ref, nqb_ref, nkvb_ref, out_hbm, max_ref, y_sem):
    group, groups = pl.program_id(0), pl.num_programs(0)
    first = lax.axis_index("tp") * groups * GROUP + group * GROUP
    y_copy = pltpu.make_async_copy(y_ref, out_hbm, y_sem)

    @pl.when(group == 0)
    def _():
        y_copy.start()
        for i in range(max_ref.shape[0]):
            max_ref[i] = top_ref[0, i]

    def gains(width, first_dim, second_is_clip):
        column = lax.broadcasted_iota(jnp.int32, (1, GROUP * width), 1)
        best, inner = jnp.full((1, GROUP * width), top_ref[0, first], f32), column
        for i in range(1, GROUP):
            best = jnp.where(column >= i * width, top_ref[0, first + i], best)
            inner = jnp.where(column >= i * width, column - i * width, inner)
        clip = CLIP_TAU / jnp.maximum(CLIP_TAU, best)
        return jnp.where(inner < first_dim, jnp.sqrt(clip), clip if second_is_clip else 1.0)

    for src, dst, width, first_dim, second_is_clip in ((wqb_ref, nqb_ref, QK, NOPE, True), (wkvb_ref, nkvb_ref, NOPE + VDIM, NOPE, False)):
        gain = gains(width, first_dim, second_is_clip)
        columns = pl.ds(pl.multiple_of(group * GROUP * width, 256), GROUP * width) if second_is_clip else slice(None)

        @pl.loop(0, src.shape[0] // 256)
        def _(i):
            here = pl.ds(pl.multiple_of(i * 256, 256), 256)
            dst[here] = (src[here, columns].astype(f32) * gain).astype(bf16)

    @pl.when(group == groups - 1)
    def _():
        y_copy.wait()


def clip(top, wqb, wkvb, y, all_heads):
    steps = wqb.shape[1] // (QK * GROUP)
    vmem = pl.BlockSpec(memory_space=pltpu.VMEM)
    qspec = pl.BlockSpec((wqb.shape[0], GROUP * QK), lambda g: (0, g))
    kvspec = pl.BlockSpec((wkvb.shape[0], GROUP * (NOPE + VDIM)), lambda g: (0, g))
    return pl.pallas_call(
        clip_kernel,
        grid=(steps,),
        in_specs=[pl.BlockSpec(memory_space=pltpu.SMEM), vmem, kvspec, vmem],
        out_specs=[qspec, kvspec, pl.BlockSpec(memory_space=pltpu.HBM), pl.BlockSpec(memory_space=pltpu.SMEM)],
        out_shape=[jax.ShapeDtypeStruct(wqb.shape, bf16), jax.ShapeDtypeStruct(wkvb.shape, bf16), jax.ShapeDtypeStruct(y.shape, bf16), jax.ShapeDtypeStruct((all_heads,), f32)],
        scratch_shapes=[pltpu.SemaphoreType.DMA],
        compiler_params=pltpu.CompilerParams(vmem_limit_bytes=10 * MIB),
        name="clip",
    )(top, in_vmem(wqb), in_hbm(wkvb), in_vmem(y))


def solution(mesh):
    def device_step(hidden, gain_in, gain_q, gain_kv, w_qa, w_kva, w_qb, w_kvb, w_out):
        x = hidden[0]
        qlat, lat, kr, tables, keep_qb = latents(x, gain_in[None], gain_q.reshape(-1, 128), gain_kv[None], w_qa, w_kva.T, rope_tables(x.shape[0]), w_qb)
        o, local_max, head = attention(qlat, lat, kr, tables, keep_qb, w_kvb, w_out)
        y, top = output_projection(o, head, w_out, x, local_max)
        new_qb, new_kvb, out, logit_max = clip(top, keep_qb, w_kvb, y, mesh.shape["tp"] * o.shape[1] // VDIM)
        return out[None], logit_max, new_qb, new_kvb

    weight_spec = P(None, 'tp')
    return jax.shard_map(device_step, mesh=mesh, in_specs=(P('dp', None, None), P(), P(), P(), P(), P(), weight_spec, weight_spec, P('tp', None)), out_specs=(P('dp', None, None), P(), weight_spec, weight_spec), check_vma=False)
```

```python
import math
import jax
import jax.numpy as jnp
import numpy as np
from jax import lax
from jax.experimental import pallas as pl
from jax.experimental.pallas import tpu as pltpu
from jax.sharding import PartitionSpec as P

NORM_EPS = 1e-6
ROPE_BASE = 50000.0
MSCALE_SQ = (0.1 * math.log(32.0) + 1.0) ** 2
CLIP_TAU = 100.0
NOPE, ROPE, VDIM = 128, 64, 128
QK = NOPE + ROPE
LOGIT_SCALE = QK ** -0.5 * MSCALE_SQ
EXP2_SCALE = LOGIT_SCALE * math.log2(math.e)
GROUP = 4
NEG = -jnp.inf
MESH = pl.DeviceIdType.MESH
MIB = 1024 * 1024
f32, bf16 = jnp.float32, jnp.bfloat16


def rope_tables(seq_len):
    inv_freq = ROPE_BASE ** (-2.0 * np.arange(ROPE // 2) / ROPE)
    angles = np.arange(seq_len)[:, None] * inv_freq[None, :]
    cos, sin = np.cos(angles), np.sin(angles)
    half, rest = np.zeros_like(sin), np.zeros((seq_len, ROPE))
    return np.stack([np.concatenate(t, axis=1) for t in ((cos, cos, rest + 1.0), (-sin, half, rest), (half, sin, rest))]).astype(np.float32)


def in_vmem(array):
    return pltpu.with_memory_space_constraint(array, pltpu.VMEM)


def in_hbm(array):
    return pltpu.with_memory_space_constraint(array, pltpu.HBM)


def turn(tensor, tables):
    return tensor * tables[0] + pltpu.roll(tensor, 96, 1) * tables[1] + pltpu.roll(tensor, 32, 1) * tables[2]


TILE = 256


def latent_kernel(x_hbm, gin_hbm, gq_hbm, gkv_hbm, wqa_hbm, wkva_hbm, tab_hbm, wqb_hbm, qlat_ref, lat_ref, kr_ref, tab_ref, wqb_ref, gin_ref, gq_ref, gkv_ref, g_sem, x_ref, n_ref, wq_ref, wkv_ref, wr_ref, full_q, full_kv, rot, scale_ref, x_sem, w_sem, send_sem, recv_sem):
    rows, dim = x_ref.shape
    tp, dp = lax.axis_index("tp"), lax.axis_index("dp")
    other = (1 - tp, dp)
    tiles, parts = wq_ref.shape[0], rows // 128
    rank = lat_ref.shape[1]

    x_copies = [pltpu.make_async_copy(x_hbm.at[pl.ds(r * 128, 128)], x_ref.at[pl.ds(r * 128, 128)], x_sem.at[r]) for r in range(parts)]
    kv_copy = pltpu.make_async_copy(wkva_hbm.at[pl.ds(pl.multiple_of(tp * TILE, TILE), TILE)], wkv_ref, w_sem.at[tiles])
    r_copy = pltpu.make_async_copy(wkva_hbm.at[pl.ds(rank, ROPE)], wr_ref, w_sem.at[tiles + 1])
    q_copies = [pltpu.make_async_copy(wqa_hbm.at[:, pl.ds(pl.multiple_of((tp * tiles + i) * TILE, TILE), TILE)], wq_ref.at[i], w_sem.at[i]) for i in range(tiles)]
    small = [pltpu.make_async_copy(src, dst, g_sem.at[i]) for i, (src, dst) in enumerate(((gin_hbm, gin_ref), (gq_hbm, gq_ref), (gkv_hbm, gkv_ref), (tab_hbm, tab_ref), (wqb_hbm, wqb_ref)))]
    for copy in [*x_copies, *small[:3]]:
        copy.start()
    barrier = pltpu.get_barrier_semaphore()
    pl.semaphore_signal(barrier, inc=1, device_id=other, device_id_type=MESH)

    def send(ref, index, slot):
        return pltpu.make_async_remote_copy(src_ref=ref.at[index], dst_ref=ref.at[index], send_sem=send_sem.at[slot], recv_sem=recv_sem.at[slot], device_id=other, device_id_type=MESH)

    half = rows // 2

    def measure(part):
        x_copies[2 * part].wait()
        x_copies[2 * part + 1].wait()

        @pl.loop(0, half // 32, unroll=4)
        def _(i):
            here = pl.ds(pl.multiple_of(part * half + i * 32, 32), 32)
            total = jnp.zeros((32, 256), f32)
            for c in range(0, dim, 256):
                v = x_ref[here, c:c + 256].astype(f32)
                total = total + v * v
            scale_ref[here] = jnp.broadcast_to(lax.rsqrt(jnp.sum(total, axis=1, keepdims=True) * (1.0 / dim) + NORM_EPS), (32, 128))

    def normalize(here):
        scale = scale_ref[here, 0:1]
        for c in range(0, dim, 256):
            n_ref[here, c:c + 256] = (x_ref[here, c:c + 256].astype(f32) * scale * gin_ref[:, c:c + 256]).astype(bf16)

    flip = (((1,), (1,)), ((), ()))
    upper, lower = slice(0, half), slice(half, rows)

    measure(0)
    q_copies[0].start()
    q_copies[1].start()
    for copy in small[:3]:
        copy.wait()

    @pl.loop(0, half // 32, unroll=2)
    def _(i):
        normalize(pl.ds(pl.multiple_of(i * 32, 32), 32))

    measure(1)
    for copy in [q_copies[2], kv_copy, r_copy, small[3]]:
        copy.start()
    q_copies[0].wait()
    q_copies[1].wait()
    for j in range(2):
        full_q[tp * tiles + j, upper] = jnp.dot(n_ref[upper], wq_ref[j], preferred_element_type=f32)
    for r in range(half, rows, 32):
        normalize(slice(r, r + 32))
    pl.semaphore_wait(barrier, 1)
    for j in range(2):
        full_q[tp * tiles + j, lower] = jnp.dot(n_ref[lower], wq_ref[j], preferred_element_type=f32)
    sends = [send(full_q, tp * tiles + j, j) for j in range(2)]
    for copy in sends:
        copy.start()
    small[4].start()
    q_copies[2].wait()
    for part in (upper, lower):
        full_q[tp * tiles + 2, part] = jnp.dot(n_ref[part], wq_ref[2], preferred_element_type=f32)
    sends.append(send(full_q, tp * tiles + 2, 2))
    sends[2].start()
    kv_copy.wait()
    r_copy.wait()
    for part in (upper, lower):
        full_kv[tp, part] = lax.dot_general(n_ref[part], wkv_ref[...], flip, preferred_element_type=f32)
    sends.append(send(full_kv, tp, tiles))
    sends[3].start()
    quarter = half // 2
    for i in range(2):
        mine = pl.ds(pl.multiple_of(tp * half + i * quarter, quarter), quarter)
        turned = lax.dot_general(n_ref[mine], wr_ref[...], flip, preferred_element_type=f32)
        rot[tp, i * quarter:i * quarter + quarter] = jnp.concatenate([turned, jnp.zeros((quarter, ROPE), f32)], axis=1)
    sends.append(send(rot, tp, tiles + 1))
    sends[4].start()
    for copy in sends[:3]:
        copy.wait()

    @pl.loop(0, rows // 32, unroll=4)
    def _(i):
        here = pl.ds(pl.multiple_of(i * 32, 32), 32)
        pieces = [full_q[j, here] for j in range(2 * tiles)]
        total = sum(a * a for a in pieces)
        scale = lax.rsqrt(jnp.sum(total, axis=1, keepdims=True) * (1.0 / (2 * tiles * TILE)) + NORM_EPS)
        for j, a in enumerate(pieces):
            qlat_ref[here, j * TILE:j * TILE + TILE] = (a * scale * jnp.concatenate([gq_ref[2 * j:2 * j + 1], gq_ref[2 * j + 1:2 * j + 2]], axis=1)).astype(bf16)

    for copy in [*sends[3:], small[3]]:
        copy.wait()
    for r in range(0, rows, 64):
        here = slice(r, r + 64)
        pieces = [full_kv[j, here] for j in range(rank // TILE)]
        total = sum(a * a for a in pieces)
        scale = lax.rsqrt(jnp.sum(total, axis=1, keepdims=True) * (1.0 / rank) + NORM_EPS)
        for j, a in enumerate(pieces):
            lat_ref[here, j * TILE:j * TILE + TILE] = (a * scale * gkv_ref[:, j * TILE:j * TILE + TILE]).astype(bf16)
        key = turn(rot[r // half, r % half:r % half + 64], [tab_ref[i, here] for i in range(3)])
        kr_ref[0, here] = key.astype(bf16)
        kr_ref[1, here] = pltpu.roll(key, 64, 1).astype(bf16)
    small[4].wait()


def latents(x, gin, gq, gkv, wqa, wkva, tables, wqb):
    rows, dim = x.shape
    q_rank, rank = wqa.shape[1], gkv.shape[1]
    tiles = q_rank // (2 * TILE)
    vmem, hbm = pl.BlockSpec(memory_space=pltpu.VMEM), pl.BlockSpec(memory_space=pltpu.HBM)
    return pl.pallas_call(
        latent_kernel,
        in_specs=[hbm] * 8,
        out_specs=[vmem] * 5,
        out_shape=[pltpu.VMEM((rows, q_rank), bf16), pltpu.VMEM((rows, rank), bf16), pltpu.VMEM((2, rows, 128), bf16), pltpu.VMEM(tables.shape, f32), pltpu.VMEM(wqb.shape, bf16)],
        scratch_shapes=[
            pltpu.VMEM(gin.shape, f32),
            pltpu.VMEM(gq.shape, f32),
            pltpu.VMEM(gkv.shape, f32),
            pltpu.SemaphoreType.DMA((5,)),
            pltpu.VMEM((rows, dim), bf16),
            pltpu.VMEM((rows, dim), bf16),
            pltpu.VMEM((tiles, dim, TILE), bf16),
            pltpu.VMEM((TILE, dim), bf16),
            pltpu.VMEM((ROPE, dim), bf16),
            pltpu.VMEM((2 * tiles, rows, TILE), f32),
            pltpu.VMEM((rank // TILE, rows, TILE), f32),
            pltpu.VMEM((2, rows // 2, 128), f32),
            pltpu.VMEM((rows, 128), f32),
            pltpu.SemaphoreType.DMA((rows // 128,)),
            pltpu.SemaphoreType.DMA((tiles + 2,)),
            pltpu.SemaphoreType.DMA((tiles + 2,)),
            pltpu.SemaphoreType.DMA((tiles + 2,)),
        ],
        compiler_params=pltpu.CompilerParams(vmem_limit_bytes=32 * MIB, collective_id=1, has_side_effects=True),
        name="latents",
    )(*(in_hbm(a) for a in (x, gin, gq, gkv, wqa, wkva, tables, wqb)))


BLOCK, CHUNK, WIDTH = 256, 32, 512


def attention_kernel(qlat_ref, lat_ref, kr_ref, tab_ref, wqb_ref, wkvb_ref, wout_hbm, o_ref, max_ref, head_ref, w_sem, mirror, *scratch):
    step, steps = pl.program_id(0), pl.num_programs(0)
    sets = (scratch[0:3], scratch[3:6])
    raws, probs = scratch[6:10], scratch[10:14]
    heads = o_ref.shape[1] // VDIM
    rows = qlat_ref.shape[0]
    lane = lax.broadcasted_iota(jnp.int32, (rows, 128), 1)

    head_copy = pltpu.make_async_copy(wout_hbm.at[:, pl.ds(0, head_ref.shape[1])], head_ref, w_sem)

    @pl.when(step == 1)
    def _():
        head_copy.start()

    @pl.when(step == steps - 1)
    def _():
        head_copy.wait()

    @pl.when(step == 0)
    def _():
        max_ref[...] = jnp.full((8, 128), NEG, f32)
        for i in range(3):
            mirror[i] = pltpu.roll(tab_ref[i], 64, 1)
        for _, keys, _ in sets:
            for h in range(0, GROUP, 2):
                keys[:, h * 256 + 128:h * 256 + 256] = kr_ref[0]
        for i, prob in enumerate(probs):
            column = 128 + i % 2 * BLOCK
            prob[0:128, column:column + 128] = jnp.zeros((128, 128), bf16)

    def project_q(buffers, n):
        queries = buffers[0]
        chunk = jnp.dot(qlat_ref[...], wqb_ref[:, pl.ds(pl.multiple_of(step * (GROUP * QK) + n * 256, 256), 256)], preferred_element_type=f32)
        for i in range(2):
            piece, kind = chunk[:, i * 128:i * 128 + 128], (2 * n + i) % 3
            if kind:
                piece = turn(piece, tab_ref if kind == 1 else mirror)
            queries[:, (2 * n + i) * 128:(2 * n + i) * 128 + 128] = piece.astype(bf16)

    def project_kv(buffers, h):
        _, keys, values = buffers
        chunk = jnp.dot(lat_ref[...], wkvb_ref[:, h * 256:h * 256 + 256], preferred_element_type=f32)
        values[:, h * VDIM:h * VDIM + VDIM] = chunk[:, NOPE:].astype(bf16)
        if h % 2:
            moved = pltpu.roll(chunk[:, :NOPE], 64, 1)
            keys[:, h * 256:h * 256 + 128] = jnp.where(lane >= 64, moved, 0.0).astype(bf16)
            keys[:, h * 256 + 128:h * 256 + 256] = jnp.where(lane < 64, moved.astype(bf16), kr_ref[1])
        else:
            keys[:, h * 256:h * 256 + 128] = chunk[:, :NOPE].astype(bf16)

    def scores(buffers, h):
        queries, keys, _ = buffers
        column = (h // 2) * 384 + (h % 2) * 128
        for b in range(2):
            hi = (b + 1) * BLOCK
            raws[2 * (h % 2) + b][:, :hi] = lax.dot_general(queries[b * BLOCK:hi, column:column + 256], keys[:hi, h * 256:h * 256 + 256], (((1,), (1,)), ((), ())), preferred_element_type=f32)

    def attend(buffers, h):
        values = buffers[2]
        peak = None
        for b in range(2):
            hi = (b + 1) * BLOCK
            raw, prob = raws[2 * (h % 2) + b], probs[2 * (h % 2) + b]
            for r in range(0, BLOCK, CHUNK):
                width = b * BLOCK + (r // 128 + 1) * 128
                tile = raw[r:r + CHUNK, :width]
                keep = lax.broadcasted_iota(jnp.int32, (CHUNK, 128), 0) + r % 128 >= lax.broadcasted_iota(jnp.int32, (CHUNK, 128), 1)
                last = jnp.where(keep, tile[:, width - 128:], NEG)
                tile = last if width == 128 else jnp.concatenate([tile[:, :width - 128], last], axis=1)
                top = jnp.max(tile, axis=1, keepdims=True)
                e = jnp.exp2(tile * EXP2_SCALE - top * EXP2_SCALE)
                prob[r:r + CHUNK, :width] = (e * (1.0 / jnp.sum(e, axis=1, keepdims=True))).astype(bf16)
                peak = top if peak is None else jnp.maximum(peak, top)
            o_ref[b * BLOCK:hi, pl.ds(pl.multiple_of((step - 1) * (GROUP * VDIM) + h * VDIM, VDIM), VDIM)] = jnp.dot(prob[:, :hi], values[:hi, h * VDIM:h * VDIM + VDIM], preferred_element_type=f32).astype(bf16)
        slot = lax.broadcasted_iota(jnp.int32, (8, 128), 1)
        index = lax.axis_index("tp") * heads + (step - 1) * GROUP + h
        max_ref[...] = jnp.where(slot == index, jnp.max(peak, axis=0, keepdims=True) * LOGIT_SCALE, max_ref[...])

    @pl.when(step == 0)
    def _():
        for n in range(3):
            project_q(sets[0], n)
        for h in range(GROUP):
            project_kv(sets[0], h)
        scores(sets[0], 0)

    for parity in range(2):
        for h in range(GROUP):
            @pl.when((step > 0) & (step < steps - 1) & (lax.rem(step, 2) == parity))
            def _():
                ahead, now = sets[parity], sets[1 - parity]
                if h < GROUP - 1:
                    project_q(ahead, h)
                    scores(now, h + 1)
                else:
                    for i in range(GROUP):
                        project_kv(ahead, i)
                    scores(ahead, 0)
                attend(now, h)

    @pl.when(step == steps - 1)
    def _():
        for h in range(GROUP):
            if h < GROUP - 1:
                scores(sets[1], h + 1)
            attend(sets[1], h)


def attention(qlat, lat, kr, tables, wqb, wkvb, w_out):
    rows = qlat.shape[0]
    heads = wqb.shape[1] // QK
    groups = heads // GROUP
    vmem, hbm = pl.BlockSpec(memory_space=pltpu.VMEM), pl.BlockSpec(memory_space=pltpu.HBM)
    buffers = [pltpu.VMEM((rows, GROUP * QK), bf16), pltpu.VMEM((rows, GROUP * 256), bf16), pltpu.VMEM((rows, GROUP * VDIM), bf16)]
    return pl.pallas_call(
        attention_kernel,
        grid=(groups + 1,),
        in_specs=[vmem, vmem, vmem, vmem, vmem, pl.BlockSpec((wkvb.shape[0], GROUP * 256), lambda g: (0, jnp.minimum(g, groups - 1))), hbm],
        out_specs=[vmem, vmem, vmem],
        out_shape=[pltpu.VMEM((rows, heads * VDIM), bf16), pltpu.VMEM((8, 128), f32), pltpu.VMEM((w_out.shape[0], WIDTH), bf16)],
        scratch_shapes=[pltpu.SemaphoreType.DMA, pltpu.VMEM(tables.shape, f32)] + buffers + buffers + [pltpu.VMEM((BLOCK, (1 + i % 2) * BLOCK), f32) for i in range(4)] + [pltpu.VMEM((BLOCK, (1 + i % 2) * BLOCK), bf16) for i in range(4)],
        compiler_params=pltpu.CompilerParams(vmem_limit_bytes=15 * MIB),
        name="attention",
    )(in_vmem(qlat), in_vmem(lat), in_vmem(kr), in_vmem(tables), in_vmem(wqb), in_hbm(wkvb), in_hbm(w_out))


def axis_peers(axis):
    dp = lax.axis_index("dp")
    stride = 4 ** axis
    here = lax.rem(dp // stride, 4)
    return [dp + (lax.rem(here + d, 4) - here) * stride for d in (1, 2, 3)]


def output_kernel(o_ref, head_ref, w_hbm, x_hbm, max_ref, y_ref, top_ref, o_buf, w_buf, part, recv, best, peer_best, x_sem, w_sem, send_sem, recv_sem, max_send, max_recv, free_sem):
    slots, rows, width = recv.shape
    blocks, depth = y_ref.shape[1] // width, w_buf.shape[0]
    tp, dp = lax.axis_index("tp"), lax.axis_index("dp")
    other = (1 - tp, dp)

    def fetch(index):
        slot = lax.rem(index, depth)
        return pltpu.make_async_copy(w_hbm.at[:, pl.ds(pl.multiple_of(index * width, width), width)], w_buf.at[slot], w_sem.at[slot])

    def x_copy(index):
        columns = pl.ds(pl.multiple_of(index * width, width), width)
        return pltpu.make_async_copy(x_hbm.at[:, columns], y_ref.at[:, columns], x_sem.at[index])

    def exchange(index):
        slot, place = lax.rem(index, 2), lax.rem(index, slots)
        return pltpu.make_async_remote_copy(src_ref=part.at[slot], dst_ref=recv.at[place], send_sem=send_sem.at[slot], recv_sem=recv_sem.at[place], device_id=other, device_id_type=MESH)

    def spread(phase, slot, device):
        return pltpu.make_async_remote_copy(
            src_ref=max_ref if phase == 0 else best.at[phase - 1], dst_ref=peer_best.at[slot], send_sem=max_send.at[slot], recv_sem=max_recv.at[slot], device_id=device, device_id_type=MESH
        )

    def phase_slots(phase):
        return [0] if phase == 0 else [1 + 3 * (phase - 1) + d for d in range(3)]

    def phase_copies(phase):
        devices = [other] if phase == 0 else [(tp, peer) for peer in axis_peers(phase - 1)]
        return [spread(phase, slot, device) for slot, device in zip(phase_slots(phase), devices)]

    def finish(index):
        columns = pl.ds(pl.multiple_of(index * width, width), width)
        for r in range(0, rows, 32):
            here = slice(r, r + 32)
            y_ref[here, columns] = (y_ref[here, columns].astype(f32) + (part[lax.rem(index, 2), here] + recv[lax.rem(index, slots), here])).astype(bf16)

    for index in range(1, depth):
        fetch(index).start()
    barrier = pltpu.get_barrier_semaphore()
    peers = [other] + [(tp, peer) for axis in range(3) for peer in axis_peers(axis)]
    for peer in peers:
        pl.semaphore_signal(barrier, inc=1, device_id=peer, device_id_type=MESH)
    pl.semaphore_wait(barrier, len(peers))
    for copy in phase_copies(0):
        copy.start()

    @pl.loop(0, rows // 32)
    def _(i):
        here = pl.ds(pl.multiple_of(i * 32, 32), 32)
        o_buf[here] = o_ref[here]

    for index in range(2):
        if index:
            fetch(index).wait()
        else:
            fetch(depth).start()
        part[index] = jnp.dot(o_buf[...], w_buf[1] if index else head_ref[...], preferred_element_type=f32)
        exchange(index).start()
        x_copy(index).start()
    fetch(depth + 1).start()

    @pl.loop(2, blocks)
    def _(index):
        for phase in range(4):
            @pl.when(index == 3 * phase + 2)
            def _():
                value = max_ref[...] if phase == 0 else best[phase - 1]
                for copy, slot in zip(phase_copies(phase), phase_slots(phase)):
                    copy.wait()
                    value = jnp.maximum(value, peer_best[slot])
                if phase < 3:
                    best[phase] = value
                else:
                    top_ref[...] = value

            if phase:
                @pl.when(index == 3 * phase)
                def _():
                    for copy in phase_copies(phase):
                        copy.start()

        x_copy(index).start()
        fetch(index).wait()
        x_copy(index - 2).wait()
        exchange(index - 2).wait()
        finish(index - 2)
        part[lax.rem(index, 2)] = jnp.dot(o_buf[...], w_buf[lax.rem(index, depth)], preferred_element_type=f32)

        @pl.when(index >= slots)
        def _():
            pl.semaphore_wait(free_sem, 1)

        exchange(index).start()

        @pl.when(index - 2 < blocks - slots)
        def _():
            pl.semaphore_signal(free_sem, inc=1, device_id=other, device_id_type=MESH)

        @pl.when(index + depth < blocks)
        def _():
            fetch(index + depth).start()

    for index in (blocks - 2, blocks - 1):
        x_copy(index).wait()
        exchange(index).wait()
        finish(index)


def output_projection(o, head, w_out, x, local_max):
    rows, depth = o.shape
    dim = w_out.shape[1]
    width = WIDTH
    slots, ring = 4, 3
    vmem, hbm = pl.BlockSpec(memory_space=pltpu.VMEM), pl.BlockSpec(memory_space=pltpu.HBM)
    return pl.pallas_call(
        output_kernel,
        in_specs=[vmem, vmem, hbm, hbm, vmem],
        out_specs=[vmem, vmem],
        out_shape=[pltpu.VMEM((rows, dim), bf16), jax.ShapeDtypeStruct((8, 128), f32)],
        scratch_shapes=[
            pltpu.VMEM(o.shape, bf16),
            pltpu.VMEM((ring, depth, width), bf16),
            pltpu.VMEM((2, rows, width), f32),
            pltpu.VMEM((slots, rows, width), f32),
            pltpu.VMEM((3, 8, 128), f32),
            pltpu.VMEM((10, 8, 128), f32),
            pltpu.SemaphoreType.DMA((dim // width,)),
            pltpu.SemaphoreType.DMA((ring,)),
            pltpu.SemaphoreType.DMA((2,)),
            pltpu.SemaphoreType.DMA((slots,)),
            pltpu.SemaphoreType.DMA((10,)),
            pltpu.SemaphoreType.DMA((10,)),
            pltpu.SemaphoreType.REGULAR,
        ],
        compiler_params=pltpu.CompilerParams(vmem_limit_bytes=23 * MIB, collective_id=0, has_side_effects=True),
        name="output_projection",
    )(in_vmem(o), in_vmem(head), in_hbm(w_out), in_hbm(x), in_vmem(local_max))


def clip_kernel(top_ref, wqb_ref, wkvb_ref, y_ref, nqb_ref, nkvb_ref, out_hbm, max_ref, y_sem):
    group, groups = pl.program_id(0), pl.num_programs(0)
    first = lax.axis_index("tp") * groups * GROUP + group * GROUP
    y_copy = pltpu.make_async_copy(y_ref, out_hbm, y_sem)

    @pl.when(group == 0)
    def _():
        y_copy.start()
        for i in range(max_ref.shape[0]):
            max_ref[i] = top_ref[0, i]

    def gains(width, first_dim, second_is_clip):
        column = lax.broadcasted_iota(jnp.int32, (1, GROUP * width), 1)
        best, inner = jnp.full((1, GROUP * width), top_ref[0, first], f32), column
        for i in range(1, GROUP):
            best = jnp.where(column >= i * width, top_ref[0, first + i], best)
            inner = jnp.where(column >= i * width, column - i * width, inner)
        clip = CLIP_TAU / jnp.maximum(CLIP_TAU, best)
        return jnp.where(inner < first_dim, jnp.sqrt(clip), clip if second_is_clip else 1.0)

    for src, dst, width, first_dim, second_is_clip in ((wqb_ref, nqb_ref, QK, NOPE, True), (wkvb_ref, nkvb_ref, NOPE + VDIM, NOPE, False)):
        gain = gains(width, first_dim, second_is_clip)
        columns = pl.ds(pl.multiple_of(group * GROUP * width, 256), GROUP * width) if second_is_clip else slice(None)

        @pl.loop(0, src.shape[0] // 256)
        def _(i):
            here = pl.ds(pl.multiple_of(i * 256, 256), 256)
            dst[here] = (src[here, columns].astype(f32) * gain).astype(bf16)

    @pl.when(group == groups - 1)
    def _():
        y_copy.wait()


def clip(top, wqb, wkvb, y, all_heads):
    steps = wqb.shape[1] // (QK * GROUP)
    vmem = pl.BlockSpec(memory_space=pltpu.VMEM)
    qspec = pl.BlockSpec((wqb.shape[0], GROUP * QK), lambda g: (0, g))
    kvspec = pl.BlockSpec((wkvb.shape[0], GROUP * (NOPE + VDIM)), lambda g: (0, g))
    return pl.pallas_call(
        clip_kernel,
        grid=(steps,),
        in_specs=[pl.BlockSpec(memory_space=pltpu.SMEM), vmem, kvspec, vmem],
        out_specs=[qspec, kvspec, pl.BlockSpec(memory_space=pltpu.HBM), pl.BlockSpec(memory_space=pltpu.SMEM)],
        out_shape=[jax.ShapeDtypeStruct(wqb.shape, bf16), jax.ShapeDtypeStruct(wkvb.shape, bf16), jax.ShapeDtypeStruct(y.shape, bf16), jax.ShapeDtypeStruct((all_heads,), f32)],
        scratch_shapes=[pltpu.SemaphoreType.DMA],
        compiler_params=pltpu.CompilerParams(vmem_limit_bytes=10 * MIB),
        name="clip",
    )(top, in_vmem(wqb), in_hbm(wkvb), in_vmem(y))


def solution(mesh):
    def device_step(hidden, gain_in, gain_q, gain_kv, w_qa, w_kva, w_qb, w_kvb, w_out):
        x = hidden[0]
        qlat, lat, kr, tables, keep_qb = latents(x, gain_in[None], gain_q.reshape(-1, 128), gain_kv[None], w_qa, w_kva.T, rope_tables(x.shape[0]), w_qb)
        o, local_max, head = attention(qlat, lat, kr, tables, keep_qb, w_kvb, w_out)
        y, top = output_projection(o, head, w_out, x, local_max)
        new_qb, new_kvb, out, logit_max = clip(top, keep_qb, w_kvb, y, mesh.shape["tp"] * o.shape[1] // VDIM)
        return out[None], logit_max, new_qb, new_kvb

    weight_spec = P(None, 'tp')
    return jax.shard_map(device_step, mesh=mesh, in_specs=(P('dp', None, None), P(), P(), P(), P(), P(), weight_spec, weight_spec, P('tp', None)), out_specs=(P('dp', None, None), P(), weight_spec, weight_spec), check_vma=False)
```

```python
import math
import jax
import jax.numpy as jnp
import numpy as np
from jax import lax
from jax.experimental import pallas as pl
from jax.experimental.pallas import tpu as pltpu
from jax.sharding import PartitionSpec as P

NORM_EPS = 1e-6
ROPE_BASE = 50000.0
MSCALE_SQ = (0.1 * math.log(32.0) + 1.0) ** 2
CLIP_TAU = 100.0
NOPE, ROPE, VDIM = 128, 64, 128
QK = NOPE + ROPE
LOGIT_SCALE = QK ** -0.5 * MSCALE_SQ
EXP2_SCALE = LOGIT_SCALE * math.log2(math.e)
GROUP = 4
NEG = -jnp.inf
MESH = pl.DeviceIdType.MESH
MIB = 1024 * 1024
f32, bf16 = jnp.float32, jnp.bfloat16


def rope_tables(seq_len):
    inv_freq = ROPE_BASE ** (-2.0 * np.arange(ROPE // 2) / ROPE)
    angles = np.arange(seq_len)[:, None] * inv_freq[None, :]
    cos, sin = np.cos(angles), np.sin(angles)
    half, rest = np.zeros_like(sin), np.zeros((seq_len, ROPE))
    return np.stack([np.concatenate(t, axis=1) for t in ((cos, cos, rest + 1.0), (-sin, half, rest), (half, sin, rest))]).astype(np.float32)


def in_vmem(array):
    return pltpu.with_memory_space_constraint(array, pltpu.VMEM)


def in_hbm(array):
    return pltpu.with_memory_space_constraint(array, pltpu.HBM)


def turn(tensor, tables):
    return tensor * tables[0] + pltpu.roll(tensor, 96, 1) * tables[1] + pltpu.roll(tensor, 32, 1) * tables[2]


TILE = 256


def latent_kernel(x_hbm, gin_hbm, gq_hbm, gkv_hbm, wqa_hbm, wkva_hbm, tab_hbm, wqb_hbm, qlat_ref, lat_ref, kr_ref, tab_ref, wqb_ref, gin_ref, gq_ref, gkv_ref, g_sem, x_ref, n_ref, wq_ref, wkv_ref, wr_ref, full_q, full_kv, rot, scale_ref, x_sem, w_sem, send_sem, recv_sem):
    rows, dim = x_ref.shape
    tp, dp = lax.axis_index("tp"), lax.axis_index("dp")
    other = (1 - tp, dp)
    tiles, parts = wq_ref.shape[0], rows // 128
    rank = lat_ref.shape[1]

    x_copies = [pltpu.make_async_copy(x_hbm.at[pl.ds(r * 128, 128)], x_ref.at[pl.ds(r * 128, 128)], x_sem.at[r]) for r in range(parts)]
    kv_copy = pltpu.make_async_copy(wkva_hbm.at[pl.ds(pl.multiple_of(tp * TILE, TILE), TILE)], wkv_ref, w_sem.at[tiles])
    r_copy = pltpu.make_async_copy(wkva_hbm.at[pl.ds(rank, ROPE)], wr_ref, w_sem.at[tiles + 1])
    q_copies = [pltpu.make_async_copy(wqa_hbm.at[:, pl.ds(pl.multiple_of((tp * tiles + i) * TILE, TILE), TILE)], wq_ref.at[i], w_sem.at[i]) for i in range(tiles)]
    small = [pltpu.make_async_copy(src, dst, g_sem.at[i]) for i, (src, dst) in enumerate(((gin_hbm, gin_ref), (gq_hbm, gq_ref), (gkv_hbm, gkv_ref), (tab_hbm, tab_ref), (wqb_hbm, wqb_ref)))]
    for copy in [*x_copies, *small[:3]]:
        copy.start()
    barrier = pltpu.get_barrier_semaphore()
    pl.semaphore_signal(barrier, inc=1, device_id=other, device_id_type=MESH)

    def send(ref, index, slot):
        return pltpu.make_async_remote_copy(src_ref=ref.at[index], dst_ref=ref.at[index], send_sem=send_sem.at[slot], recv_sem=recv_sem.at[slot], device_id=other, device_id_type=MESH)

    half = rows // 2

    def measure(part):
        x_copies[2 * part].wait()
        x_copies[2 * part + 1].wait()

        @pl.loop(0, half // 32, unroll=4)
        def _(i):
            here = pl.ds(pl.multiple_of(part * half + i * 32, 32), 32)
            total = jnp.zeros((32, 256), f32)
            for c in range(0, dim, 256):
                v = x_ref[here, c:c + 256].astype(f32)
                total = total + v * v
            scale_ref[here] = jnp.broadcast_to(lax.rsqrt(jnp.sum(total, axis=1, keepdims=True) * (1.0 / dim) + NORM_EPS), (32, 128))

    def normalize(here):
        scale = scale_ref[here, 0:1]
        for c in range(0, dim, 256):
            n_ref[here, c:c + 256] = (x_ref[here, c:c + 256].astype(f32) * scale * gin_ref[:, c:c + 256]).astype(bf16)

    flip = (((1,), (1,)), ((), ()))
    upper, lower = slice(0, half), slice(half, rows)

    measure(0)
    q_copies[0].start()
    q_copies[1].start()
    for copy in small[:3]:
        copy.wait()

    @pl.loop(0, half // 32, unroll=2)
    def _(i):
        normalize(pl.ds(pl.multiple_of(i * 32, 32), 32))

    measure(1)
    for copy in [q_copies[2], kv_copy, r_copy, small[3]]:
        copy.start()
    q_copies[0].wait()
    q_copies[1].wait()
    for j in range(2):
        full_q[tp * tiles + j, upper] = jnp.dot(n_ref[upper], wq_ref[j], preferred_element_type=f32)
    for r in range(half, rows, 32):
        normalize(slice(r, r + 32))
    pl.semaphore_wait(barrier, 1)
    for j in range(2):
        full_q[tp * tiles + j, lower] = jnp.dot(n_ref[lower], wq_ref[j], preferred_element_type=f32)
    sends = [send(full_q, tp * tiles + j, j) for j in range(2)]
    for copy in sends:
        copy.start()
    small[4].start()
    q_copies[2].wait()
    for part in (upper, lower):
        full_q[tp * tiles + 2, part] = jnp.dot(n_ref[part], wq_ref[2], preferred_element_type=f32)
    sends.append(send(full_q, tp * tiles + 2, 2))
    sends[2].start()
    kv_copy.wait()
    r_copy.wait()
    for part in (upper, lower):
        full_kv[tp, part] = lax.dot_general(n_ref[part], wkv_ref[...], flip, preferred_element_type=f32)
    sends.append(send(full_kv, tp, tiles))
    sends[3].start()
    quarter = half // 2
    for i in range(2):
        mine = pl.ds(pl.multiple_of(tp * half + i * quarter, quarter), quarter)
        turned = lax.dot_general(n_ref[mine], wr_ref[...], flip, preferred_element_type=f32)
        rot[tp, i * quarter:i * quarter + quarter] = jnp.concatenate([turned, jnp.zeros((quarter, ROPE), f32)], axis=1)
    sends.append(send(rot, tp, tiles + 1))
    sends[4].start()
    for copy in sends[:3]:
        copy.wait()

    @pl.loop(0, rows // 32, unroll=4)
    def _(i):
        here = pl.ds(pl.multiple_of(i * 32, 32), 32)
        pieces = [full_q[j, here] for j in range(2 * tiles)]
        total = sum(a * a for a in pieces)
        scale = lax.rsqrt(jnp.sum(total, axis=1, keepdims=True) * (1.0 / (2 * tiles * TILE)) + NORM_EPS)
        for j, a in enumerate(pieces):
            qlat_ref[here, j * TILE:j * TILE + TILE] = (a * scale * jnp.concatenate([gq_ref[2 * j:2 * j + 1], gq_ref[2 * j + 1:2 * j + 2]], axis=1)).astype(bf16)

    for copy in [*sends[3:], small[3]]:
        copy.wait()
    for r in range(0, rows, 64):
        here = slice(r, r + 64)
        pieces = [full_kv[j, here] for j in range(rank // TILE)]
        total = sum(a * a for a in pieces)
        scale = lax.rsqrt(jnp.sum(total, axis=1, keepdims=True) * (1.0 / rank) + NORM_EPS)
        for j, a in enumerate(pieces):
            lat_ref[here, j * TILE:j * TILE + TILE] = (a * scale * gkv_ref[:, j * TILE:j * TILE + TILE]).astype(bf16)
        key = turn(rot[r // half, r % half:r % half + 64], [tab_ref[i, here] for i in range(3)])
        kr_ref[0, here] = key.astype(bf16)
        kr_ref[1, here] = pltpu.roll(key, 64, 1).astype(bf16)
    small[4].wait()


def latents(x, gin, gq, gkv, wqa, wkva, tables, wqb):
    rows, dim = x.shape
    q_rank, rank = wqa.shape[1], gkv.shape[1]
    tiles = q_rank // (2 * TILE)
    vmem, hbm = pl.BlockSpec(memory_space=pltpu.VMEM), pl.BlockSpec(memory_space=pltpu.HBM)
    return pl.pallas_call(
        latent_kernel,
        in_specs=[hbm] * 8,
        out_specs=[vmem] * 5,
        out_shape=[pltpu.VMEM((rows, q_rank), bf16), pltpu.VMEM((rows, rank), bf16), pltpu.VMEM((2, rows, 128), bf16), pltpu.VMEM(tables.shape, f32), pltpu.VMEM(wqb.shape, bf16)],
        scratch_shapes=[
            pltpu.VMEM(gin.shape, f32),
            pltpu.VMEM(gq.shape, f32),
            pltpu.VMEM(gkv.shape, f32),
            pltpu.SemaphoreType.DMA((5,)),
            pltpu.VMEM((rows, dim), bf16),
            pltpu.VMEM((rows, dim), bf16),
            pltpu.VMEM((tiles, dim, TILE), bf16),
            pltpu.VMEM((TILE, dim), bf16),
            pltpu.VMEM((ROPE, dim), bf16),
            pltpu.VMEM((2 * tiles, rows, TILE), f32),
            pltpu.VMEM((rank // TILE, rows, TILE), f32),
            pltpu.VMEM((2, rows // 2, 128), f32),
            pltpu.VMEM((rows, 128), f32),
            pltpu.SemaphoreType.DMA((rows // 128,)),
            pltpu.SemaphoreType.DMA((tiles + 2,)),
            pltpu.SemaphoreType.DMA((tiles + 2,)),
            pltpu.SemaphoreType.DMA((tiles + 2,)),
        ],
        compiler_params=pltpu.CompilerParams(vmem_limit_bytes=32 * MIB, collective_id=1, has_side_effects=True),
        name="latents",
    )(*(in_hbm(a) for a in (x, gin, gq, gkv, wqa, wkva, tables, wqb)))


BLOCK, CHUNK, WIDTH = 256, 32, 512


def attention_kernel(qlat_ref, lat_ref, kr_ref, tab_ref, wqb_ref, wkvb_ref, wout_hbm, o_ref, max_ref, head_ref, w_sem, mirror, *scratch):
    step, steps = pl.program_id(0), pl.num_programs(0)
    sets = (scratch[0:3], scratch[3:6])
    raws, probs = scratch[6:10], scratch[10:14]
    heads = o_ref.shape[1] // VDIM
    rows = qlat_ref.shape[0]
    lane = lax.broadcasted_iota(jnp.int32, (rows, 128), 1)

    head_copy = pltpu.make_async_copy(wout_hbm.at[:, pl.ds(0, head_ref.shape[1])], head_ref, w_sem)

    @pl.when(step == 1)
    def _():
        head_copy.start()

    @pl.when(step == steps - 1)
    def _():
        head_copy.wait()

    @pl.when(step == 0)
    def _():
        max_ref[...] = jnp.full((8, 128), NEG, f32)
        for i in range(3):
            mirror[i] = pltpu.roll(tab_ref[i], 64, 1)
        for _, keys, _ in sets:
            for h in range(0, GROUP, 2):
                keys[:, h * 256 + 128:h * 256 + 256] = kr_ref[0]
        for i, prob in enumerate(probs):
            column = 128 + i % 2 * BLOCK
            prob[0:128, column:column + 128] = jnp.zeros((128, 128), bf16)

    def project_q(buffers, n):
        queries = buffers[0]
        chunk = jnp.dot(qlat_ref[...], wqb_ref[:, pl.ds(pl.multiple_of(step * (GROUP * QK) + n * 256, 256), 256)], preferred_element_type=f32)
        for i in range(2):
            piece, kind = chunk[:, i * 128:i * 128 + 128], (2 * n + i) % 3
            if kind:
                piece = turn(piece, tab_ref if kind == 1 else mirror)
            queries[:, (2 * n + i) * 128:(2 * n + i) * 128 + 128] = piece.astype(bf16)

    def project_kv(buffers, h):
        _, keys, values = buffers
        chunk = jnp.dot(lat_ref[...], wkvb_ref[:, h * 256:h * 256 + 256], preferred_element_type=f32)
        values[:, h * VDIM:h * VDIM + VDIM] = chunk[:, NOPE:].astype(bf16)
        if h % 2:
            moved = pltpu.roll(chunk[:, :NOPE], 64, 1)
            keys[:, h * 256:h * 256 + 128] = jnp.where(lane >= 64, moved, 0.0).astype(bf16)
            keys[:, h * 256 + 128:h * 256 + 256] = jnp.where(lane < 64, moved.astype(bf16), kr_ref[1])
        else:
            keys[:, h * 256:h * 256 + 128] = chunk[:, :NOPE].astype(bf16)

    def scores(buffers, h):
        queries, keys, _ = buffers
        column = (h // 2) * 384 + (h % 2) * 128
        for b in range(2):
            hi = (b + 1) * BLOCK
            raws[2 * (h % 2) + b][:, :hi] = lax.dot_general(queries[b * BLOCK:hi, column:column + 256], keys[:hi, h * 256:h * 256 + 256], (((1,), (1,)), ((), ())), preferred_element_type=f32)

    def attend(buffers, h):
        values = buffers[2]
        peak = None
        for b in range(2):
            hi = (b + 1) * BLOCK
            raw, prob = raws[2 * (h % 2) + b], probs[2 * (h % 2) + b]
            for r in range(0, BLOCK, CHUNK):
                width = b * BLOCK + (r // 128 + 1) * 128
                tile = raw[r:r + CHUNK, :width]
                keep = lax.broadcasted_iota(jnp.int32, (CHUNK, 128), 0) + r % 128 >= lax.broadcasted_iota(jnp.int32, (CHUNK, 128), 1)
                last = jnp.where(keep, tile[:, width - 128:], NEG)
                tile = last if width == 128 else jnp.concatenate([tile[:, :width - 128], last], axis=1)
                top = jnp.max(tile, axis=1, keepdims=True)
                e = jnp.exp2(tile * EXP2_SCALE - top * EXP2_SCALE)
                prob[r:r + CHUNK, :width] = (e * (1.0 / jnp.sum(e, axis=1, keepdims=True))).astype(bf16)
                peak = top if peak is None else jnp.maximum(peak, top)
            o_ref[b * BLOCK:hi, pl.ds(pl.multiple_of((step - 1) * (GROUP * VDIM) + h * VDIM, VDIM), VDIM)] = jnp.dot(prob[:, :hi], values[:hi, h * VDIM:h * VDIM + VDIM], preferred_element_type=f32).astype(bf16)
        slot = lax.broadcasted_iota(jnp.int32, (8, 128), 1)
        index = lax.axis_index("tp") * heads + (step - 1) * GROUP + h
        max_ref[...] = jnp.where(slot == index, jnp.max(peak, axis=0, keepdims=True) * LOGIT_SCALE, max_ref[...])

    @pl.when(step == 0)
    def _():
        for n in range(3):
            project_q(sets[0], n)
        for h in range(GROUP):
            project_kv(sets[0], h)
        scores(sets[0], 0)

    for parity in range(2):
        for h in range(GROUP):
            @pl.when((step > 0) & (step < steps - 1) & (lax.rem(step, 2) == parity))
            def _():
                ahead, now = sets[parity], sets[1 - parity]
                if h < GROUP - 1:
                    project_q(ahead, h)
                    scores(now, h + 1)
                else:
                    for i in range(GROUP):
                        project_kv(ahead, i)
                    scores(ahead, 0)
                attend(now, h)

    @pl.when(step == steps - 1)
    def _():
        for h in range(GROUP):
            if h < GROUP - 1:
                scores(sets[1], h + 1)
            attend(sets[1], h)


def attention(qlat, lat, kr, tables, wqb, wkvb, w_out):
    rows = qlat.shape[0]
    heads = wqb.shape[1] // QK
    groups = heads // GROUP
    vmem, hbm = pl.BlockSpec(memory_space=pltpu.VMEM), pl.BlockSpec(memory_space=pltpu.HBM)
    buffers = [pltpu.VMEM((rows, GROUP * QK), bf16), pltpu.VMEM((rows, GROUP * 256), bf16), pltpu.VMEM((rows, GROUP * VDIM), bf16)]
    return pl.pallas_call(
        attention_kernel,
        grid=(groups + 1,),
        in_specs=[vmem, vmem, vmem, vmem, vmem, pl.BlockSpec((wkvb.shape[0], GROUP * 256), lambda g: (0, jnp.minimum(g, groups - 1))), hbm],
        out_specs=[vmem, vmem, vmem],
        out_shape=[pltpu.VMEM((rows, heads * VDIM), bf16), pltpu.VMEM((8, 128), f32), pltpu.VMEM((w_out.shape[0], WIDTH), bf16)],
        scratch_shapes=[pltpu.SemaphoreType.DMA, pltpu.VMEM(tables.shape, f32)] + buffers + buffers + [pltpu.VMEM((BLOCK, (1 + i % 2) * BLOCK), f32) for i in range(4)] + [pltpu.VMEM((BLOCK, (1 + i % 2) * BLOCK), bf16) for i in range(4)],
        compiler_params=pltpu.CompilerParams(vmem_limit_bytes=15 * MIB),
        name="attention",
    )(in_vmem(qlat), in_vmem(lat), in_vmem(kr), in_vmem(tables), in_vmem(wqb), in_hbm(wkvb), in_hbm(w_out))


def axis_peers(axis):
    dp = lax.axis_index("dp")
    stride = 4 ** axis
    here = lax.rem(dp // stride, 4)
    return [dp + (lax.rem(here + d, 4) - here) * stride for d in (1, 2, 3)]


def output_kernel(o_ref, head_ref, w_hbm, x_hbm, max_ref, y_ref, top_ref, o_buf, w_buf, part, recv, best, peer_best, x_sem, w_sem, send_sem, recv_sem, max_send, max_recv, half_send, half_recv, free_sem):
    slots, rows, width = recv.shape
    blocks, depth = y_ref.shape[1] // width, w_buf.shape[0]
    tp, dp = lax.axis_index("tp"), lax.axis_index("dp")
    other = (1 - tp, dp)

    def fetch(index):
        slot = lax.rem(index, depth)
        return pltpu.make_async_copy(w_hbm.at[:, pl.ds(pl.multiple_of(index * width, width), width)], w_buf.at[slot], w_sem.at[slot])

    def x_copy(index):
        columns = pl.ds(pl.multiple_of(index * width, width), width)
        return pltpu.make_async_copy(x_hbm.at[:, columns], y_ref.at[:, columns], x_sem.at[index])

    def exchange(index):
        slot, place = lax.rem(index, 2), lax.rem(index, slots)
        return pltpu.make_async_remote_copy(src_ref=part.at[slot], dst_ref=recv.at[place], send_sem=send_sem.at[slot], recv_sem=recv_sem.at[place], device_id=other, device_id_type=MESH)

    def spread(phase, slot, device):
        return pltpu.make_async_remote_copy(
            src_ref=max_ref if phase == 0 else best.at[phase - 1], dst_ref=peer_best.at[slot], send_sem=max_send.at[slot], recv_sem=max_recv.at[slot], device_id=device, device_id_type=MESH
        )

    def phase_slots(phase):
        return [0] if phase == 0 else [1 + 3 * (phase - 1) + d for d in range(3)]

    def phase_copies(phase):
        devices = [other] if phase == 0 else [(tp, peer) for peer in axis_peers(phase - 1)]
        return [spread(phase, slot, device) for slot, device in zip(phase_slots(phase), devices)]

    def finish(index, start=0, stop=None):
        columns = pl.ds(pl.multiple_of(index * width, width), width)
        for r in range(start, stop or rows, 32):
            here = slice(r, r + 32)
            y_ref[here, columns] = (y_ref[here, columns].astype(f32) + (part[lax.rem(index, 2), here] + recv[lax.rem(index, slots), here])).astype(bf16)

    for index in range(1, depth):
        fetch(index).start()
    barrier = pltpu.get_barrier_semaphore()
    peers = [other] + [(tp, peer) for axis in range(3) for peer in axis_peers(axis)]
    for peer in peers:
        pl.semaphore_signal(barrier, inc=1, device_id=peer, device_id_type=MESH)

    @pl.loop(0, rows // 32)
    def _(i):
        here = pl.ds(pl.multiple_of(i * 32, 32), 32)
        o_buf[here] = o_ref[here]

    for index in range(2):
        if index:
            fetch(index).wait()
        else:
            fetch(depth).start()
        part[index] = jnp.dot(o_buf[...], w_buf[1] if index else head_ref[...], preferred_element_type=f32)
        if index == 0:
            pl.semaphore_wait(barrier, len(peers))
            for copy in phase_copies(0):
                copy.start()
        exchange(index).start()
        x_copy(index).start()
    fetch(depth + 1).start()

    def gather_max(phase):
        value = max_ref[...] if phase == 0 else best[phase - 1]
        for copy, slot in zip(phase_copies(phase), phase_slots(phase)):
            copy.wait()
            value = jnp.maximum(value, peer_best[slot])
        if phase < 3:
            best[phase] = value
        else:
            top_ref[...] = value

    @pl.loop(2, blocks - 1)
    def _(index):
        for phase in range(3):
            @pl.when(index == 3 * phase + 2)
            def _():
                gather_max(phase)

            @pl.when(index == 3 * phase + 3)
            def _():
                for copy in phase_copies(phase + 1):
                    copy.start()

        x_copy(index).start()
        fetch(index).wait()
        x_copy(index - 2).wait()
        exchange(index - 2).wait()
        finish(index - 2)
        part[lax.rem(index, 2)] = jnp.dot(o_buf[...], w_buf[lax.rem(index, depth)], preferred_element_type=f32)

        @pl.when(index >= slots)
        def _():
            pl.semaphore_wait(free_sem, 1)

        exchange(index).start()

        @pl.when(index - 2 < blocks - slots)
        def _():
            pl.semaphore_signal(free_sem, inc=1, device_id=other, device_id_type=MESH)

        @pl.when(index + depth < blocks)
        def _():
            fetch(index + depth).start()

    last, half = blocks - 1, rows // 2

    def exchange_half(i):
        here = pl.ds(i * half, half)
        return pltpu.make_async_remote_copy(
            src_ref=part.at[last % 2, here], dst_ref=recv.at[last % slots, here], send_sem=half_send.at[i], recv_sem=half_recv.at[i], device_id=other, device_id_type=MESH
        )

    gather_max(3)
    x_copy(last).start()
    fetch(last).wait()
    x_copy(last - 2).wait()
    exchange(last - 2).wait()
    finish(last - 2)
    for i in range(2):
        here = slice(i * half, i * half + half)
        part[last % 2, here] = jnp.dot(o_buf[here], w_buf[last % depth], preferred_element_type=f32)
        if i == 0:
            pl.semaphore_wait(free_sem, 1)
        exchange_half(i).start()
    x_copy(last - 1).wait()
    exchange(last - 1).wait()
    finish(last - 1)
    x_copy(last).wait()
    for i in range(2):
        exchange_half(i).wait()
        finish(last, i * half, i * half + half)


def output_projection(o, head, w_out, x, local_max):
    rows, depth = o.shape
    dim = w_out.shape[1]
    width = WIDTH
    slots, ring = 4, 3
    vmem, hbm = pl.BlockSpec(memory_space=pltpu.VMEM), pl.BlockSpec(memory_space=pltpu.HBM)
    return pl.pallas_call(
        output_kernel,
        in_specs=[vmem, vmem, hbm, hbm, vmem],
        out_specs=[vmem, vmem],
        out_shape=[pltpu.VMEM((rows, dim), bf16), jax.ShapeDtypeStruct((8, 128), f32)],
        scratch_shapes=[
            pltpu.VMEM(o.shape, bf16),
            pltpu.VMEM((ring, depth, width), bf16),
            pltpu.VMEM((2, rows, width), f32),
            pltpu.VMEM((slots, rows, width), f32),
            pltpu.VMEM((3, 8, 128), f32),
            pltpu.VMEM((10, 8, 128), f32),
            pltpu.SemaphoreType.DMA((dim // width,)),
            pltpu.SemaphoreType.DMA((ring,)),
            pltpu.SemaphoreType.DMA((2,)),
            pltpu.SemaphoreType.DMA((slots,)),
            pltpu.SemaphoreType.DMA((10,)),
            pltpu.SemaphoreType.DMA((10,)),
            pltpu.SemaphoreType.DMA((2,)),
            pltpu.SemaphoreType.DMA((2,)),
            pltpu.SemaphoreType.REGULAR,
        ],
        compiler_params=pltpu.CompilerParams(vmem_limit_bytes=23 * MIB, collective_id=0, has_side_effects=True),
        name="output_projection",
    )(in_vmem(o), in_vmem(head), in_hbm(w_out), in_hbm(x), in_vmem(local_max))


def clip_kernel(top_ref, wqb_ref, wkvb_ref, y_ref, nqb_ref, nkvb_ref, out_hbm, max_ref, y_sem):
    group, groups = pl.program_id(0), pl.num_programs(0)
    first = lax.axis_index("tp") * groups * GROUP + group * GROUP
    y_copy = pltpu.make_async_copy(y_ref, out_hbm, y_sem)

    @pl.when(group == 0)
    def _():
        y_copy.start()
        for i in range(max_ref.shape[0]):
            max_ref[i] = top_ref[0, i]

    def gains(width, first_dim, second_is_clip):
        column = lax.broadcasted_iota(jnp.int32, (1, GROUP * width), 1)
        best, inner = jnp.full((1, GROUP * width), top_ref[0, first], f32), column
        for i in range(1, GROUP):
            best = jnp.where(column >= i * width, top_ref[0, first + i], best)
            inner = jnp.where(column >= i * width, column - i * width, inner)
        clip = CLIP_TAU / jnp.maximum(CLIP_TAU, best)
        return jnp.where(inner < first_dim, jnp.sqrt(clip), clip if second_is_clip else 1.0)

    for src, dst, width, first_dim, second_is_clip in ((wqb_ref, nqb_ref, QK, NOPE, True), (wkvb_ref, nkvb_ref, NOPE + VDIM, NOPE, False)):
        gain = gains(width, first_dim, second_is_clip)
        columns = pl.ds(pl.multiple_of(group * GROUP * width, 256), GROUP * width) if second_is_clip else slice(None)

        @pl.loop(0, src.shape[0] // 256)
        def _(i):
            here = pl.ds(pl.multiple_of(i * 256, 256), 256)
            dst[here] = (src[here, columns].astype(f32) * gain).astype(bf16)

    @pl.when(group == groups - 1)
    def _():
        y_copy.wait()


def clip(top, wqb, wkvb, y, all_heads):
    steps = wqb.shape[1] // (QK * GROUP)
    vmem = pl.BlockSpec(memory_space=pltpu.VMEM)
    qspec = pl.BlockSpec((wqb.shape[0], GROUP * QK), lambda g: (0, g))
    kvspec = pl.BlockSpec((wkvb.shape[0], GROUP * (NOPE + VDIM)), lambda g: (0, g))
    return pl.pallas_call(
        clip_kernel,
        grid=(steps,),
        in_specs=[pl.BlockSpec(memory_space=pltpu.SMEM), vmem, kvspec, vmem],
        out_specs=[qspec, kvspec, pl.BlockSpec(memory_space=pltpu.HBM), pl.BlockSpec(memory_space=pltpu.SMEM)],
        out_shape=[jax.ShapeDtypeStruct(wqb.shape, bf16), jax.ShapeDtypeStruct(wkvb.shape, bf16), jax.ShapeDtypeStruct(y.shape, bf16), jax.ShapeDtypeStruct((all_heads,), f32)],
        scratch_shapes=[pltpu.SemaphoreType.DMA],
        compiler_params=pltpu.CompilerParams(vmem_limit_bytes=10 * MIB),
        name="clip",
    )(top, in_vmem(wqb), in_hbm(wkvb), in_vmem(y))


def solution(mesh):
    def device_step(hidden, gain_in, gain_q, gain_kv, w_qa, w_kva, w_qb, w_kvb, w_out):
        x = hidden[0]
        qlat, lat, kr, tables, keep_qb = latents(x, gain_in[None], gain_q.reshape(-1, 128), gain_kv[None], w_qa, w_kva.T, rope_tables(x.shape[0]), w_qb)
        o, local_max, head = attention(qlat, lat, kr, tables, keep_qb, w_kvb, w_out)
        y, top = output_projection(o, head, w_out, x, local_max)
        new_qb, new_kvb, out, logit_max = clip(top, keep_qb, w_kvb, y, mesh.shape["tp"] * o.shape[1] // VDIM)
        return out[None], logit_max, new_qb, new_kvb

    weight_spec = P(None, 'tp')
    return jax.shard_map(device_step, mesh=mesh, in_specs=(P('dp', None, None), P(), P(), P(), P(), P(), weight_spec, weight_spec, P('tp', None)), out_specs=(P('dp', None, None), P(), weight_spec, weight_spec), check_vma=False)
```
